32 devices in a mesh: replica: 2 (over x), tp: 16 (over z, y, core).
Axes of the slice: x: 2, y: 2, z: 4, core: 2. Of those that a mesh axis runs over, the one named last changes fastest.
Arguments:
- hidden_in: bfloat16 [8, 16384], P('replica', 'tp'), parts along dimension 0, may hold values from -60 to 60
- norm_gain: bfloat16 [16384], P('tp'), may hold values from 0.5 to 1.5
- w_qkv: bfloat16 [16384, 9216], P(None, 'tp'), may hold values from -0.046875 to 0.046875
- w_out: bfloat16 [8192, 16384], P('tp'), may hold values from -0.09375 to 0.09375
- key_cache: bfloat16 [8, 2048, 512], P('replica', 'tp'), parts along dimension 0, may hold values from -1200 to 1200
- value_cache: bfloat16 [8, 2048, 512], P('replica', 'tp'), parts along dimension 0, may hold values from -6 to 6
- lengths: int32 [8], P('replica'), parts along dimension 0, may hold values from 1024 to 2048
- positions: int32 [8], P('replica'), parts along dimension 0, may hold values from 0 to 4095
Outputs:
- attn_out: bfloat16 [8, 16384], P('replica', 'tp'), parts along dimension 0
- token_scale: float32 [8], P('replica'), parts along dimension 0
The draws below stay inside these ranges and needn't reach their ends.
There are 2 independent parts, one for each index of `replica`. The reference program is written for one: setup_inputs(seed, part) draws one part's arguments, and reference() takes and returns one part's arrays. A program takes and returns all parts, laid end to end along the dimension named above; an argument that names none is the same for every part. Nothing has to cross between parts.
All inputs are finite; a program needn't handle non-finite values.
Results may differ from the reference program's by a relative error of at most 0.017.
The reference program's roundings to bfloat16 on the way count: a program that leaves them out, or rounds other values in their place, can miss the bound.
Values may be sent and summed in bfloat16 or wider, within the bound.
A program may use at most 128 MiB of HBM per device.

```python
import jax
import jax.numpy as jnp
from jax import lax

D = 16384
QUERY_HEADS = 64
KEY_VALUE_HEADS = 4
HEAD_SIZE = 128
BATCH_SEQUENCES = 4
DEVICE_POSITIONS = 128
CACHE_POSITIONS = 2048
QKVW = 9216


def draw_hidden_in(key, part):
    leading_part, second = jax.random.split(key, 2)
    column = jnp.exp(jax.random.uniform(second, (D,), jnp.float32, 0.0, jnp.log(10.0)))
    values = jnp.clip(jax.random.normal(leading_part, (BATCH_SEQUENCES, D), jnp.float32), -6.0, 6.0) * column[None, :]
    return jnp.clip(values, -60.0, 60.0).astype(jnp.bfloat16)


def draw_key_cache(key, part):
    leading_part = jax.random.fold_in(key, 0)
    offset_start = jnp.clip(jax.random.normal(leading_part, (BATCH_SEQUENCES, CACHE_POSITIONS, KEY_VALUE_HEADS * HEAD_SIZE), jnp.float32), -6.0, 6.0)
    return jnp.clip(offset_start, -1200.0, 1200.0).astype(jnp.bfloat16)


def touch_ends(entries, rng, smallest, high):
    index_at = [jax.random.randint(jax.random.fold_in(rng, axis), (), 0, length) for axis, length in enumerate(entries.shape)]
    longest = entries.shape.index(max(entries.shape))
    next_to = index_at[:longest] + [(index_at[longest] + 1) % entries.shape[longest]] + index_at[longest + 1:]
    return entries.at[tuple(index_at)].set(smallest).at[tuple(next_to)].set(high)


def raised(result, key, source, target, blocks, factor):
    owner, partner = [(jnp.arange(result.shape[axis_at]) // (result.shape[axis_at] // blocks)).reshape([-1 if axis == axis_at else 1 for axis in range(result.ndim)]) for axis_at in (source, target)]
    chosen = jax.random.permutation(key, blocks)[partner]
    strong = (owner == chosen) | (owner == (partner + blocks // 2) % blocks)
    return jnp.where(strong, factor * result, result)


def levels(own_key, dims, pieces, smallest, high):
    factor_of, own = 1.0, jax.random.fold_in(own_key, 6)
    for dim, shards_of in pieces:
        steps = jnp.exp(jax.random.uniform(jax.random.fold_in(own, dim), (shards_of,), jnp.float32, smallest / len(pieces), high / len(pieces)))
        factor_of = factor_of * jnp.repeat(steps, dims[dim] // shards_of).reshape([-1 if axis == dim else 1 for axis in range(len(dims))])
    return factor_of


def gaussian(rng, shape, scale, limit, pieces=(), kind=jnp.bfloat16):
    gain = levels(rng, shape, pieces, -0.22, 0.18) if pieces else 1.0
    values = jax.random.normal(rng, shape, jnp.float32) * scale * gain
    return jnp.minimum(jnp.maximum(values, -limit), limit).astype(kind)


def gaussian_with(own_key, shape, scale, bound, cuts, heavy, kind=jnp.bfloat16):
    drawn = scale * jax.random.normal(own_key, shape, jnp.float32)
    if cuts:
        drawn = drawn * levels(own_key, shape, cuts, -0.22, 0.18)
    return jnp.clip(raised(drawn, jax.random.fold_in(own_key, 3), *heavy), -bound, bound).astype(kind)


def setup_inputs(seed: int = 0, part: int = 0) -> dict:
    keys = jax.random.split(jax.random.key(seed), 9)
    own_keys = jax.random.split(jax.random.fold_in(keys[8], part), 9)
    hidden_in = draw_hidden_in(jax.random.fold_in(jax.random.fold_in(keys[8], part), 71), part)
    norm_gain = jnp.clip(1.0 + 0.1 * jax.random.normal(keys[1], (D,), jnp.float32), 0.5, 1.5).astype(jnp.bfloat16)
    w_qkv = gaussian(keys[2], (D, QKVW), D ** -0.5, 0.046875, ((1, 16),))
    w_out = gaussian_with(keys[3], (QUERY_HEADS * HEAD_SIZE, D), (QUERY_HEADS * HEAD_SIZE) ** -0.5, 0.09375, ((0, 16),), (0, 1, 16, 2.0))
    key_cache = draw_key_cache(jax.random.fold_in(jax.random.fold_in(keys[8], part), 71), part)
    value_cache = gaussian(own_keys[5], (BATCH_SEQUENCES, CACHE_POSITIONS, KEY_VALUE_HEADS * HEAD_SIZE), 1.0, 6.0, ((1, 16),))
    lengths = touch_ends(jax.random.randint(own_keys[6], (BATCH_SEQUENCES,), CACHE_POSITIONS // 2, CACHE_POSITIONS + 1), jax.random.fold_in(own_keys[6], 1), CACHE_POSITIONS // 2, CACHE_POSITIONS).astype(jnp.int32)
    positions = touch_ends(jax.random.randint(own_keys[7], (BATCH_SEQUENCES,), 0, 2 * CACHE_POSITIONS), jax.random.fold_in(own_keys[7], 1), 0, (2 * CACHE_POSITIONS) - 1).astype(jnp.int32)
    return dict(hidden_in=hidden_in, norm_gain=norm_gain, w_qkv=w_qkv, w_out=w_out, key_cache=key_cache, value_cache=value_cache, lengths=lengths, positions=positions)


def apply_rotation(heads, positions):
    half = HEAD_SIZE // 2
    freq = 500000.0 ** (-(jnp.arange(half, dtype=jnp.float32) * 2.0) / HEAD_SIZE)
    angle = positions.astype(jnp.float32)[:, None] * freq[None, :]
    cosine = jnp.cos(angle)[:, None, :]
    sine = jnp.sin(angle)[:, None, :]
    leading_part = heads[..., :half]
    second = heads[..., half:]
    return jnp.concatenate([leading_part * cosine - second * sine, second * cosine + leading_part * sine], axis=-1)

def reference(hidden_in, norm_gain, w_qkv, w_out, key_cache, value_cache, lengths, positions):
    batch_count = hidden_in.shape[0]
    group_count = QUERY_HEADS // KEY_VALUE_HEADS
    block_list = CACHE_POSITIONS // DEVICE_POSITIONS
    query_width = QUERY_HEADS * HEAD_SIZE
    key_width = KEY_VALUE_HEADS * HEAD_SIZE
    inv = 1.0 / HEAD_SIZE ** 0.5
    values = hidden_in.astype(jnp.float32)
    rstd = lax.rsqrt(lax.optimization_barrier(jnp.mean(values * values, axis=-1)) + 1e-05)
    normed = values * norm_gain.astype(jnp.float32)[None, :] * rstd[:, None]
    token_scale = (lax.optimization_barrier(jnp.max(jnp.abs(normed), axis=-1)) + 1e-06) / 448.0
    quant = (normed / token_scale[:, None]).astype(jnp.bfloat16)
    query_key_value = (jnp.dot(quant, w_qkv, preferred_element_type=jnp.float32) * token_scale[:, None]).astype(jnp.bfloat16)
    query_rows = apply_rotation(query_key_value[:, :query_width].astype(jnp.float32).reshape(batch_count, QUERY_HEADS, HEAD_SIZE), positions).astype(jnp.bfloat16)
    latest_key = apply_rotation(query_key_value[:, query_width:query_width + key_width].astype(jnp.float32).reshape(batch_count, KEY_VALUE_HEADS, HEAD_SIZE), positions)
    latest_value = query_key_value[:, query_width + key_width:].astype(jnp.float32).reshape(batch_count, KEY_VALUE_HEADS, HEAD_SIZE)
    grouped_query = query_rows.astype(jnp.float32).reshape(batch_count, KEY_VALUE_HEADS, group_count, HEAD_SIZE)
    key_rows = key_cache.astype(jnp.float32).reshape(batch_count, block_list, DEVICE_POSITIONS, KEY_VALUE_HEADS, HEAD_SIZE)
    value_rows = value_cache.astype(jnp.float32).reshape(batch_count, block_list, DEVICE_POSITIONS, KEY_VALUE_HEADS, HEAD_SIZE)
    scores = jnp.einsum('bgjd,bnpgd->bgjnp', grouped_query, key_rows) * inv
    where_pos = jnp.arange(CACHE_POSITIONS, dtype=jnp.int32).reshape(block_list, DEVICE_POSITIONS)
    valid = (where_pos[None, :, :] < lengths[:, None, None])[:, None, None, :, :]
    block_max = lax.optimization_barrier(jnp.max(jnp.where(valid, scores, -1e+30), axis=-1))
    weights = jnp.where(valid, jnp.exp(scores - block_max[..., None]), 0.0)
    block_sum = lax.optimization_barrier(jnp.sum(weights, axis=-1))
    rounded = lax.optimization_barrier(weights.astype(jnp.bfloat16)).astype(jnp.float32)
    block_out = jnp.einsum('bgjnp,bnpgd->bgjnd', rounded, value_rows)
    top = lax.optimization_barrier(jnp.max(block_max, axis=-1))
    factor = jnp.exp(block_max - top[..., None])
    total = lax.optimization_barrier(jnp.sum(block_sum * factor, axis=-1))
    summed = lax.optimization_barrier(jnp.sum(block_out * factor[..., None], axis=-2))
    score_new = jnp.einsum('bgjd,bgd->bgj', grouped_query, latest_key) * inv
    top_new = jnp.maximum(top, score_new)
    keep = jnp.exp(top - top_new)
    fresh = jnp.exp(score_new - top_new)
    total = total * keep + fresh
    summed = summed * keep[..., None] + fresh[..., None] * latest_value[:, :, None, :]
    att = (summed / total[..., None]).reshape(batch_count, query_width).astype(jnp.bfloat16)
    attn_out = jnp.dot(att, w_out, preferred_element_type=jnp.float32).astype(jnp.bfloat16)
    return (attn_out, token_scale)
```

```python
import functools

import jax
import jax.numpy as jnp
import numpy as np
from jax import lax
from jax.experimental import pallas as pl
from jax.experimental.pallas import tpu as pltpu
from jax.sharding import PartitionSpec as P

QUERY_HEADS = 64
KEY_VALUE_HEADS = 4
HEAD_SIZE = 128
LANES = 128


def rounded_up(value, step):
    return (value + step - 1) // step * step


def partner(me, k, n):
    peer = me
    bit = 1
    while bit < n:
        if isinstance(k, int):
            if k & bit:
                peer = peer + (bit - 2 * bit * ((me // bit) % 2))
        else:
            mine, flip = (me // bit) % 2, (k // bit) % 2
            peer = peer + bit * flip * (1 - 2 * mine)
        bit *= 2
    return peer


def kernel(
    n,
    hidden_hbm,
    gain_hbm,
    wq_hbm,
    wo_hbm,
    key_hbm,
    value_hbm,
    lens_hbm,
    pos_hbm,
    freq_hbm,
    out_ref,
    scale_ref,
    xg,
    quant,
    wq,
    wo,
    kv,
    vv,
    stats,
    stage,
    qg,
    heads,
    so,
    og,
    sl,
    lg,
    rs_send,
    rs_recv,
    lens_ref,
    pos_ref,
    freq_ref,
    local_sem,
    wq_sem,
    wo_sem,
    kv_sem,
    t_send,
    t_recv,
    x_send,
    x_recv,
    q_send,
    q_recv,
    o_send,
    o_recv,
    l_send,
    l_recv,
    r_send,
    r_recv,
):
    me = lax.axis_index("tp")
    dx = wo.shape[1] // n
    batch = lens_ref.shape[0]
    pieces = dx // LANES
    x_rows = pieces * batch
    gain_at = xg.shape[1] - rounded_up(pieces, 8)
    cw, width = wq_hbm.shape
    blocks = stage.shape[0] // batch
    padded = blocks * LANES
    own_rows = og.shape[1]
    own_heads = own_rows // batch
    positions = key_hbm.shape[1]
    group = QUERY_HEADS // KEY_VALUE_HEADS
    f32, bf16 = jnp.float32, jnp.bfloat16
    unrolled = n <= 16

    per = 4
    groups = n // per
    span_of = lambda base: pl.ds(pl.multiple_of(base * dx, per * dx), per * dx)

    def base_of(i):
        return partner(me, i * per, n) // per * per

    def wq_copy(i):
        span = span_of(base_of(i))
        return pltpu.make_async_copy(wq_hbm.at[:, span], wq.at[:, span], wq_sem.at[i])

    def wo_copy(i):
        span = span_of(base_of(i))
        return pltpu.make_async_copy(wo_hbm.at[:, span], wo.at[:, span], wo_sem.at[i])

    def remote(src, dst, send, recv, peer):
        return pltpu.make_async_remote_copy(
            src_ref=src,
            dst_ref=dst,
            send_sem=send,
            recv_sem=recv,
            device_id={"tp": peer},
            device_id_type=pl.DeviceIdType.MESH,
        )

    def far_first(act):
        if unrolled:
            for k in range(n - 1, 0, -1):
                act(k, partner(me, k, n))
        else:

            def step(i, carry):
                act(n - 1 - i, partner(me, n - 1 - i, n))
                return carry

            lax.fori_loop(0, n - 1, step, 0)

    def all_sent(ref, send, recv):
        part = ref.at[pl.ds(0, n - 1)]
        remote(part, part, send, recv, partner(me, 1, n)).wait_send()

    def all_received(ref, send, recv, count=n - 1):
        part = ref.at[pl.ds(0, count)]
        remote(part, part, send, recv, partner(me, 1, n)).wait_recv()

    small = [
        (hidden_hbm, xg.at[me, pl.ds(0, x_rows), :]),
        (gain_hbm, xg.at[me, pl.ds(gain_at, pieces), :]),
        (freq_hbm, freq_ref),
        (pos_hbm, pos_ref),
        (lens_hbm, lens_ref),
    ]
    small = [
        pltpu.make_async_copy(src, dst, local_sem.at[i]) for i, (src, dst) in enumerate(small)
    ]
    for copy in small:
        copy.start()

    barrier = pltpu.get_barrier_semaphore()
    far_first(
        lambda k, peer: pl.semaphore_signal(
            barrier, inc=1, device_id={"tp": peer}, device_id_type=pl.DeviceIdType.MESH
        )
    )
    copy_k = pltpu.make_async_copy(key_hbm, kv, kv_sem.at[0])
    copy_v = pltpu.make_async_copy(value_hbm, vv, kv_sem.at[1])

    small[0].wait()
    small[1].wait()

    half8 = lax.broadcasted_iota(jnp.int32, (8, LANES), 0) // batch
    row4 = lax.broadcasted_iota(jnp.int32, (8, LANES), 0) % batch
    lane8 = lax.broadcasted_iota(jnp.int32, (8, LANES), 1)
    per8 = 8 // batch

    def gained(s):
        x = xg[s, 0:x_rows, :].astype(f32)
        g = xg[s, gain_at : gain_at + rounded_up(pieces, 8), :].astype(f32)
        xs, ys = [], []
        for j in range(x_rows // 8):
            x8 = x[8 * j : 8 * j + 8, :]
            g8 = jnp.zeros((8, LANES), f32)
            for u in range(per8):
                r = j * per8 + u
                g8 = jnp.where(half8 == u, g[r : r + 1, :], g8)
            xs.append(x8)
            ys.append(x8 * g8)
        return xs, ys

    xs, ys = gained(me)
    squares = sum(x8 * x8 for x8 in xs)
    peak = functools.reduce(jnp.maximum, [jnp.abs(y) for y in ys])
    squares = jnp.sum(squares, axis=-1, keepdims=True)
    peak = jnp.max(peak, axis=-1, keepdims=True)
    first = jnp.sum(jnp.where(lane8 == row4, squares, 0.0), axis=0, keepdims=True)
    second = jnp.max(jnp.where(lane8 == row4 + batch, peak, 0.0), axis=0, keepdims=True)
    stats[me] = jnp.where(lane8[0:1, :] < batch, first, second)

    for i in range(groups):
        wq_copy(i).start()

    pl.semaphore_wait(barrier, n - 1)

    far_first(
        lambda k, peer: remote(stats.at[me], stats.at[me], t_send, t_recv, peer).start()
    )
    far_first(
        lambda k, peer: remote(xg.at[me], xg.at[me], x_send, x_recv.at[k // per], peer).start()
    )

    for copy in small[2:]:
        copy.wait()
    place = jnp.zeros((8, LANES), f32)
    for b in range(batch):
        place = jnp.where(row4 == b, pos_ref[b].astype(f32), place)
    angle = place * freq_ref[...]
    cosine = jnp.cos(angle)
    sine = jnp.sin(angle)
    sine = jnp.where(lane8 < HEAD_SIZE // 2, -sine, sine)

    all_received(stats, t_send, t_recv)
    if n % 8 == 0:
        rows = [stats[8 * i : 8 * i + 8, 0, :] for i in range(n // 8)]
        added = jnp.sum(sum(rows), axis=0, keepdims=True)
        largest = jnp.max(functools.reduce(jnp.maximum, rows), axis=0, keepdims=True)
    else:
        rows = [stats[i] for i in range(n)]
        added = sum(rows)
        largest = functools.reduce(jnp.maximum, rows)
    added = jnp.sum(jnp.where(lane8 == row4, added, 0.0), axis=-1, keepdims=True)
    largest = jnp.max(jnp.where(lane8 == row4 + batch, largest, 0.0), axis=-1, keepdims=True)
    rstd8 = lax.rsqrt(added / width + 1e-05)
    scale8 = (largest * rstd8 + 1e-06) / 448.0
    token_scale = scale8[0:batch, :]
    scale_ref[...] = jnp.sum(
        jnp.where((lane8 == row4) & (half8 == 0), scale8, 0.0), axis=0, keepdims=True
    )[:, 0:batch]
    rstd8 = jnp.broadcast_to(rstd8, (8, LANES))
    scale8 = jnp.broadcast_to(scale8, (8, LANES))

    copy_k.start()
    copy_v.start()
    for i in range(groups - 1, -1, -1):
        wo_copy(i).start()

    all_received(xg, x_send, x_recv.at[0], per - 1)

    def project(i, acc):
        base = base_of(i)
        wq_copy(i).wait()

        @pl.when(i > 0)
        def _():
            all_received(xg, x_send, x_recv.at[i], per)

        for u in range(per):
            _, ys = gained(base + u)
            rows = [y * rstd8 / scale8 for y in ys]
            flat = [row[v * batch : (v + 1) * batch, :] for row in rows for v in range(per8)]
            span = pl.ds(pl.multiple_of((base + u) * dx, dx), dx)
            quant[:, span] = jnp.concatenate(flat, axis=1).astype(bf16)
        span = span_of(base)
        return acc + lax.dot_general(
            wq[:, span], quant[:, span], (((1,), (1,)), ((), ())), preferred_element_type=f32
        )

    acc = lax.fori_loop(0, groups, project, jnp.zeros((cw, batch), f32))
    proj = (acc.T * token_scale).astype(bf16).astype(f32)
    if padded > cw:
        proj = jnp.concatenate([proj, jnp.zeros((batch, padded - cw), f32)], axis=1)
    if cw % LANES:
        proj = pltpu.roll(proj, lax.rem(me * cw, LANES), 1)
    for j in range(blocks):
        stage[j * batch : (j + 1) * batch, :] = proj[:, j * LANES : (j + 1) * LANES]
    qg[me, 0 : blocks * batch, :] = stage[...].astype(bf16)
    far_first(lambda k, peer: remote(qg.at[me], qg.at[me], q_send, q_recv, peer).start())
    copy_k.wait()
    copy_v.wait()
    all_received(qg, q_send, q_recv)

    total_heads = QUERY_HEADS + 2 * KEY_VALUE_HEADS
    unpacked = [qg[d].astype(f32) for d in range(n)]
    for h in range(total_heads):
        piece = None
        for d in range(h * LANES // cw, (h * LANES + LANES - 1) // cw + 1):
            block = h - d * cw // LANES
            part = unpacked[d][block * batch : (block + 1) * batch, :]
            piece = part if piece is None else piece + part
        heads[h * batch : (h + 1) * batch, :] = piece

    def rotated(rows):
        count = rows.shape[0]
        turned = pltpu.roll(rows, HEAD_SIZE // 2, 1)
        return rows * jnp.tile(cosine, (count // 8, 1)) + turned * jnp.tile(sine, (count // 8, 1))

    inv = 1.0 / HEAD_SIZE**0.5
    rows_g = group * batch
    cols = batch * positions
    col = lax.broadcasted_iota(jnp.int32, (8, cols), 1)
    row = lax.broadcasted_iota(jnp.int32, (8, cols), 0)
    limit = jnp.zeros((8, cols), jnp.int32)
    for b in range(batch):
        limit = jnp.where(col // positions == b, lens_ref[b], limit)
    valid8 = (row % batch == col // positions) & (me * positions + col % positions < limit)
    bias8 = jnp.where(valid8, 0.0, -1e30)
    bias = jnp.tile(bias8, (rows_g // 8, 1))
    valid = bias == 0.0
    fresh_rows = rotated(
        heads[QUERY_HEADS * batch : (QUERY_HEADS + KEY_VALUE_HEADS) * batch, :]
    )
    own_lane = lax.broadcasted_iota(jnp.int32, (own_rows, LANES), 1)
    own_row = lax.broadcasted_iota(jnp.int32, (own_rows, LANES), 0)
    diagonal = own_lane == own_row
    for g in range(KEY_VALUE_HEADS):
        q = rotated(heads[g * rows_g : (g + 1) * rows_g, :]).astype(bf16)
        k_rows = kv[:, :, g * HEAD_SIZE : (g + 1) * HEAD_SIZE].reshape(cols, HEAD_SIZE)
        v_rows = vv[:, :, g * HEAD_SIZE : (g + 1) * HEAD_SIZE].reshape(cols, HEAD_SIZE)
        s = (
            lax.dot_general(q, k_rows, (((1,), (1,)), ((), ())), preferred_element_type=f32) * inv
        )
        top = jnp.max(jnp.where(valid, s, -1e30), axis=-1, keepdims=True)
        w = jnp.where(valid, jnp.exp(s - top), 0.0)
        total = jnp.sum(w, axis=-1, keepdims=True)
        o = jnp.dot(w.astype(bf16), v_rows, preferred_element_type=f32)
        k_new = fresh_rows[g * batch : (g + 1) * batch, :]
        base = (QUERY_HEADS + KEY_VALUE_HEADS + g) * batch
        v_new = heads[base : base + batch, :]
        s_new = (
            jnp.sum(q.astype(f32) * jnp.tile(k_new, (group, 1)), axis=-1, keepdims=True) * inv
        )
        s_new = jnp.where(me == 0, s_new, -1e30)
        top_new = jnp.maximum(top, s_new)
        keep = jnp.exp(top - top_new)
        fresh = jnp.where(me == 0, jnp.exp(s_new - top_new), 0.0)
        total = total * keep + fresh
        o = o * keep + fresh * jnp.tile(v_new, (group, 1))
        some = total > 0.0
        safe = jnp.where(some, total, 1.0)
        o = (o / safe).astype(bf16)
        lse = jnp.where(some, top_new + jnp.log(safe), -1e30)
        for j in range(group // own_heads):
            e = g * (group // own_heads) + j
            so[e] = o[j * own_rows : (j + 1) * own_rows, :]
            sl[e] = jnp.sum(
                jnp.where(diagonal, lse[j * own_rows : (j + 1) * own_rows, :], 0.0),
                axis=0,
                keepdims=True,
            )

    def send_o(k, peer):
        remote(so.at[peer], og.at[me], o_send, o_recv, peer).start()
        remote(sl.at[peer], lg.at[me], l_send, l_recv, peer).start()

    far_first(send_o)
    og[me] = so[me]
    lg[me] = sl[me]
    for i in range(groups):
        wo_copy(i).wait()

    all_received(lg, l_send, l_recv)
    all_received(og, o_send, o_recv)

    lses = [
        jnp.sum(jnp.where(diagonal, lg[s], 0.0), axis=-1, keepdims=True) for s in range(n)
    ]
    best = functools.reduce(jnp.maximum, lses)
    den = jnp.zeros_like(best)
    num = jnp.zeros((own_rows, LANES), f32)
    for s in range(n):
        share = jnp.exp(lses[s] - best)
        den = den + share
        num = num + share * og[s].astype(f32)
    att = num / den
    att = jnp.concatenate(
        [att[j * batch : (j + 1) * batch, :] for j in range(own_heads)], axis=1
    ).astype(bf16)

    def rows_of(part):
        return jnp.concatenate(
            [part[:, j * LANES : (j + 1) * LANES] for j in range(pieces)], axis=0
        )

    def send_part(peer, part):
        rs_send[peer] = rows_of(part).astype(bf16)
        remote(rs_send.at[peer], rs_recv.at[me], r_send, r_recv, peer).start()

    def project_out(j, carry):
        i = groups - 1 - j
        base = base_of(i)
        parts = jnp.dot(att, wo[:, span_of(base)], preferred_element_type=f32)
        for u in range(per):
            send_part(base + u, parts[:, u * dx : (u + 1) * dx])
        return carry

    lax.fori_loop(0, groups - 1, project_out, 0)

    def out_of(peer):
        span = pl.ds(pl.multiple_of(peer * dx, dx), dx)
        return jnp.dot(att, wo[:, span], preferred_element_type=f32)

    near = [partner(me, k, n) for k in range(per - 1, 0, -1)]
    parts = [out_of(peer) for peer in near]
    for peer, part in zip(near, parts):
        send_part(peer, part)
    own = rows_of(out_of(me))

    all_received(rs_recv, r_send, r_recv)
    total = own
    if unrolled:
        for k in range(1, n):
            total = total + rs_recv[partner(me, k, n)].astype(f32)
    else:
        total = lax.fori_loop(
            1, n, lambda k, t: t + rs_recv[partner(me, k, n)].astype(f32), total
        )
    out_ref[...] = total.astype(bf16)

    all_sent(stats, t_send, t_recv)
    all_sent(xg, x_send, x_recv.at[0])
    all_sent(qg, q_send, q_recv)
    all_sent(so, o_send, o_recv)
    all_sent(sl, l_send, l_recv)
    all_sent(rs_send, r_send, r_recv)


def hand_over(result_ref, scale_ref, out_ref, token_scale_ref):
    out_ref[...] = result_ref[...]
    token_scale_ref[...] = scale_ref[...]


def on_device(n, hidden_in, norm_gain, w_qkv, w_out, key_cache, value_cache, lengths, positions):
    batch, dx = hidden_in.shape
    cw = w_qkv.shape[1]
    own_rows = w_out.shape[0] // HEAD_SIZE * batch
    total_heads = QUERY_HEADS + 2 * KEY_VALUE_HEADS
    widest = max(d * cw % LANES for d in range(n)) + cw
    blocks = rounded_up(widest, LANES) // LANES
    pieces = dx // LANES
    x_height = rounded_up(pieces * batch, 8) + rounded_up(pieces, 8)
    half = HEAD_SIZE // 2
    freq = np.float32(500000.0) ** (
        -(np.arange(half, dtype=np.float32) * np.float32(2.0)) / np.float32(HEAD_SIZE)
    )
    freq = jnp.asarray(np.tile(freq.astype(np.float32), 2)[None, :])
    bf16, f32 = jnp.bfloat16, jnp.float32
    dma = pltpu.SemaphoreType.DMA
    hbm = pl.BlockSpec(memory_space=pl.ANY)
    vmem = pl.BlockSpec(memory_space=pltpu.VMEM)
    out, token_scale = pl.pallas_call(
        functools.partial(kernel, n),
        out_shape=(
            jax.ShapeDtypeStruct((pieces * batch, LANES), bf16),
            jax.ShapeDtypeStruct((1, batch), f32),
        ),
        in_specs=[hbm] * 9,
        out_specs=(vmem, vmem),
        scratch_shapes=[
            pltpu.VMEM((n, x_height, LANES), bf16),
            pltpu.VMEM((batch, n * dx), bf16),
            pltpu.VMEM((cw, n * dx), bf16),
            pltpu.VMEM((w_out.shape[0], n * dx), bf16),
            pltpu.VMEM(key_cache.shape, bf16),
            pltpu.VMEM(value_cache.shape, bf16),
            pltpu.VMEM((n, 1, LANES), f32),
            pltpu.VMEM((blocks * batch, LANES), f32),
            pltpu.VMEM((n, rounded_up(blocks * batch, 8), LANES), bf16),
            pltpu.VMEM((total_heads * batch, HEAD_SIZE), f32),
            pltpu.VMEM((n, own_rows, LANES), bf16),
            pltpu.VMEM((n, own_rows, LANES), bf16),
            pltpu.VMEM((n, 1, LANES), f32),
            pltpu.VMEM((n, 1, LANES), f32),
            pltpu.VMEM((n, pieces * batch, LANES), bf16),
            pltpu.VMEM((n, pieces * batch, LANES), bf16),
            pltpu.SMEM((batch,), jnp.int32),
            pltpu.SMEM((batch,), jnp.int32),
            pltpu.VMEM((1, LANES), f32),
            dma((5,)),
            dma((n // 4,)),
            dma((n // 4,)),
            dma((2,)),
            dma(()),
            dma(()),
            dma(()),
            dma((n // 4,)),
        ]
        + [dma(())] * 8,
        compiler_params=pltpu.CompilerParams(
            collective_id=0, has_side_effects=True, vmem_limit_bytes=60 * 1024 * 1024
        ),
        name="decode",
    )(
        hidden_in.reshape(batch, pieces, LANES).transpose(1, 0, 2).reshape(-1, LANES),
        norm_gain.reshape(dx // LANES, LANES),
        w_qkv.T,
        w_out,
        key_cache,
        value_cache,
        lengths,
        positions,
        freq,
    )
    out, token_scale = pl.pallas_call(
        hand_over,
        out_shape=(
            jax.ShapeDtypeStruct(out.shape, out.dtype),
            jax.ShapeDtypeStruct(token_scale.shape, token_scale.dtype),
        ),
        in_specs=[vmem, vmem],
        out_specs=(vmem, vmem),
        name="hand_over",
    )(out, token_scale)
    out = out.reshape(pieces, batch, LANES).transpose(1, 0, 2).reshape(batch, dx)
    return out, token_scale.reshape(batch)


def solution(mesh):
    placed = (
        P("replica", "tp"),
        P("tp"),
        P(None, "tp"),
        P("tp", None),
        P("replica", "tp", None),
        P("replica", "tp", None),
        P("replica"),
        P("replica"),
    )
    return jax.shard_map(
        functools.partial(on_device, mesh.shape["tp"]),
        mesh=mesh,
        in_specs=placed,
        out_specs=(P("replica", "tp"), P("replica")),
        check_vma=False,
    )
```

```python
import functools

import jax
import jax.numpy as jnp
import numpy as np
from jax import lax
from jax.experimental import pallas as pl
from jax.experimental.pallas import tpu as pltpu
from jax.sharding import PartitionSpec as P

QUERY_HEADS = 64
KEY_VALUE_HEADS = 4
HEAD_SIZE = 128
LANES = 128


def rounded_up(value, step):
    return (value + step - 1) // step * step


def partner(me, k, n):
    peer = me
    bit = 1
    while bit < n:
        if isinstance(k, int):
            if k & bit:
                peer = peer + (bit - 2 * bit * ((me // bit) % 2))
        else:
            mine, flip = (me // bit) % 2, (k // bit) % 2
            peer = peer + bit * flip * (1 - 2 * mine)
        bit *= 2
    return peer


def kernel(
    n,
    hidden_hbm,
    gain_hbm,
    wq_hbm,
    wo_hbm,
    key_hbm,
    value_hbm,
    lens_hbm,
    pos_hbm,
    freq_hbm,
    out_ref,
    scale_ref,
    xg,
    quant,
    wq,
    wt,
    wz,
    wo,
    kv,
    vv,
    stats,
    qg,
    heads,
    ordered,
    so,
    og,
    sl,
    lg,
    rs_send,
    rs_recv,
    lens_ref,
    pos_ref,
    freq_ref,
    local_sem,
    wq_sem,
    wo_sem,
    kv_sem,
    t_send,
    t_recv,
    x_send,
    x_recv,
    q_send,
    q_recv,
    o_send,
    o_recv,
    l_send,
    l_recv,
    r_send,
    r_recv,
):
    me = lax.axis_index("tp")
    dx = wo.shape[1] // n
    batch = lens_ref.shape[0]
    pieces = dx // LANES
    x_rows = pieces * batch
    gain_at = xg.shape[1] - rounded_up(pieces, 8)
    cw, width = wq_hbm.shape
    padded = qg.shape[2]
    own_rows = og.shape[1]
    own_heads = own_rows // batch
    positions = key_hbm.shape[1]
    group = QUERY_HEADS // KEY_VALUE_HEADS
    f32, bf16 = jnp.float32, jnp.bfloat16
    unrolled = n <= 16

    per = 4
    groups = n // per
    span_of = lambda base: pl.ds(pl.multiple_of(base * dx, per * dx), per * dx)

    def base_of(i):
        return partner(me, i * per, n) // per * per

    half = per // 2
    turned = wt.shape[1]

    def half_of(i):
        return pl.multiple_of(partner(me, i * half, n) // half * half * dx, half * dx)

    def wq_copy(i):
        span = pl.ds(half_of(i), half * dx)
        return pltpu.make_async_copy(wq_hbm.at[:, span], wq.at[:, span], wq_sem.at[i])

    def turn_into(ref, i, place):
        start = half_of(i)
        for j in range(half * dx // LANES):
            at = pl.multiple_of(start + j * LANES, LANES)
            to = pl.multiple_of(place * half * dx + j * LANES, LANES)
            ref[pl.ds(to, LANES), :] = wq[0:turned, pl.ds(at, LANES)].T

    def turn(i, carry):
        wq_copy(i).wait()
        turn_into(wt, i, i)
        return carry

    def wo_copy(i):
        span = span_of(base_of(i))
        return pltpu.make_async_copy(wo_hbm.at[:, span], wo.at[:, span], wo_sem.at[i])

    def remote(src, dst, send, recv, peer):
        return pltpu.make_async_remote_copy(
            src_ref=src,
            dst_ref=dst,
            send_sem=send,
            recv_sem=recv,
            device_id={"tp": peer},
            device_id_type=pl.DeviceIdType.MESH,
        )

    def far_first(act):
        if unrolled:
            for k in range(n - 1, 0, -1):
                act(k, partner(me, k, n))
        else:

            def step(i, carry):
                act(n - 1 - i, partner(me, n - 1 - i, n))
                return carry

            lax.fori_loop(0, n - 1, step, 0)

    def all_sent(ref, send, recv):
        part = ref.at[pl.ds(0, n - 1)]
        remote(part, part, send, recv, partner(me, 1, n)).wait_send()

    def all_received(ref, send, recv, count=n - 1):
        part = ref.at[pl.ds(0, count)]
        remote(part, part, send, recv, partner(me, 1, n)).wait_recv()

    small = [
        (hidden_hbm, xg.at[me, pl.ds(0, x_rows), :]),
        (gain_hbm, xg.at[me, pl.ds(gain_at, pieces), :]),
        (freq_hbm, freq_ref),
        (pos_hbm, pos_ref),
        (lens_hbm, lens_ref),
    ]
    small = [
        pltpu.make_async_copy(src, dst, local_sem.at[i]) for i, (src, dst) in enumerate(small)
    ]
    for copy in small:
        copy.start()

    barrier = pltpu.get_barrier_semaphore()
    far_first(
        lambda k, peer: pl.semaphore_signal(
            barrier, inc=1, device_id={"tp": peer}, device_id_type=pl.DeviceIdType.MESH
        )
    )
    copy_k = pltpu.make_async_copy(key_hbm, kv, kv_sem.at[0])
    copy_v = pltpu.make_async_copy(value_hbm, vv, kv_sem.at[1])

    small[0].wait()
    small[1].wait()

    half8 = lax.broadcasted_iota(jnp.int32, (8, LANES), 0) // batch
    row4 = lax.broadcasted_iota(jnp.int32, (8, LANES), 0) % batch
    lane8 = lax.broadcasted_iota(jnp.int32, (8, LANES), 1)
    per8 = 8 // batch

    def gained(s):
        x = xg[s, 0:x_rows, :].astype(f32)
        g = xg[s, gain_at : gain_at + rounded_up(pieces, 8), :].astype(f32)
        xs, ys = [], []
        for j in range(x_rows // 8):
            x8 = x[8 * j : 8 * j + 8, :]
            g8 = jnp.zeros((8, LANES), f32)
            for u in range(per8):
                r = j * per8 + u
                g8 = jnp.where(half8 == u, g[r : r + 1, :], g8)
            xs.append(x8)
            ys.append(x8 * g8)
        return xs, ys

    xs, ys = gained(me)
    squares = sum(x8 * x8 for x8 in xs)
    peak = functools.reduce(jnp.maximum, [jnp.abs(y) for y in ys])
    squares = jnp.sum(squares, axis=-1, keepdims=True)
    peak = jnp.max(peak, axis=-1, keepdims=True)
    first = jnp.sum(jnp.where(lane8 == row4, squares, 0.0), axis=0, keepdims=True)
    second = jnp.max(jnp.where(lane8 == row4 + batch, peak, 0.0), axis=0, keepdims=True)
    stats[me] = jnp.where(lane8[0:1, :] < batch, first, second)

    for i in range(2 * groups):
        wq_copy(i).start()
    early = 1
    lax.fori_loop(0, early, turn, 0)

    pl.semaphore_wait(barrier, n - 1)

    far_first(
        lambda k, peer: remote(stats.at[me], stats.at[me], t_send, t_recv, peer).start()
    )
    far_first(
        lambda k, peer: remote(xg.at[me], xg.at[me], x_send, x_recv.at[k // per], peer).start()
    )

    for copy in small[2:]:
        copy.wait()
    place = jnp.zeros((8, LANES), f32)
    for b in range(batch):
        place = jnp.where(row4 == b, pos_ref[b].astype(f32), place)
    angle = place * freq_ref[...]
    cosine = jnp.cos(angle)
    sine = jnp.sin(angle)
    sine = jnp.where(lane8 < HEAD_SIZE // 2, -sine, sine)

    lax.fori_loop(early, 2 * groups - 2, turn, 0)
    all_received(stats, t_send, t_recv)
    if n % 8 == 0:
        rows = [stats[8 * i : 8 * i + 8, 0, :] for i in range(n // 8)]
        added = jnp.sum(sum(rows), axis=0, keepdims=True)
        largest = jnp.max(functools.reduce(jnp.maximum, rows), axis=0, keepdims=True)
    else:
        rows = [stats[i] for i in range(n)]
        added = sum(rows)
        largest = functools.reduce(jnp.maximum, rows)
    added = jnp.sum(jnp.where(lane8 == row4, added, 0.0), axis=-1, keepdims=True)
    largest = jnp.max(jnp.where(lane8 == row4 + batch, largest, 0.0), axis=-1, keepdims=True)
    rstd8 = lax.rsqrt(added / width + 1e-05)
    scale8 = (largest * rstd8 + 1e-06) / 448.0
    token_scale = scale8[0:batch, :]
    scale_ref[...] = jnp.sum(
        jnp.where((lane8 == row4) & (half8 == 0), scale8, 0.0), axis=0, keepdims=True
    )[:, 0:batch]
    rstd8 = jnp.broadcast_to(rstd8, (8, LANES))
    scale8 = jnp.broadcast_to(scale8, (8, LANES))

    copy_k.start()
    copy_v.start()
    for i in range(groups - 1, -1, -1):
        wo_copy(i).start()

    def project(i, carry, ref, place):
        acc, rest = carry
        for v in range(2):
            first = half_of(2 * i + v) // dx
            for u in range(half):
                _, ys = gained(first + u)
                rows = [y * rstd8 / scale8 for y in ys]
                flat = [row[w * batch : (w + 1) * batch, :] for row in rows for w in range(per8)]
                quant[2 * i + v, :, u * dx : (u + 1) * dx] = jnp.concatenate(
                    flat, axis=1
                ).astype(bf16)
        for v in range(2):
            x = quant[2 * i + v]
            to = pl.multiple_of((2 * place + v) * half * dx, half * dx)
            acc = acc + jnp.dot(x, ref[pl.ds(to, half * dx), :], preferred_element_type=f32)
            if turned < cw:
                rest = rest + lax.dot_general(
                    wq[turned:cw, pl.ds(half_of(2 * i + v), half * dx)],
                    x,
                    (((1,), (1,)), ((), ())),
                    preferred_element_type=f32,
                )
        return acc, rest

    def project_middle(i, carry):
        all_received(xg, x_send, x_recv.at[i], per)
        return project(i, carry, wt, i)

    carry = (jnp.zeros((batch, turned), f32), jnp.zeros((cw - turned, batch), f32))
    for i in range(2):
        wq_copy(2 * groups - 2 + i).wait()
        all_received(xg, x_send, x_recv.at[i], per if i else per - 1)
        turn_into(wz, 2 * groups - 2 + i, i)
        carry = project(i, carry, wt, i)
    carry = lax.fori_loop(2, groups - 1, project_middle, carry)
    all_received(xg, x_send, x_recv.at[groups - 1], per)
    acc, rest = project(groups - 1, carry, wz, 0)
    if turned < cw:
        acc = jnp.concatenate([acc, rest.T], axis=1)
    proj = (acc * token_scale).astype(bf16).astype(f32)
    if padded > cw:
        proj = jnp.concatenate([proj, jnp.zeros((batch, padded - cw), f32)], axis=1)
    if cw % LANES:
        proj = pltpu.roll(proj, lax.rem(me * cw, LANES), 1)
    qg[me] = proj.astype(bf16)
    far_first(lambda k, peer: remote(qg.at[me], qg.at[me], q_send, q_recv, peer).start())
    copy_k.wait()
    copy_v.wait()
    all_received(qg, q_send, q_recv)

    total_heads = QUERY_HEADS + 2 * KEY_VALUE_HEADS
    unpacked = [qg[d].astype(f32) for d in range(n)]
    for h in range(total_heads):
        piece = None
        for d in range(h * LANES // cw, (h * LANES + LANES - 1) // cw + 1):
            block = h - d * cw // LANES
            part = unpacked[d][:, block * LANES : (block + 1) * LANES]
            piece = part if piece is None else piece + part
        heads[h * batch : (h + 1) * batch, :] = piece

    inv = 1.0 / HEAD_SIZE**0.5

    def row_of(rows, b):
        return jnp.broadcast_to(rows[b : b + 1, :], (group, HEAD_SIZE))

    cosines = [row_of(cosine, b) for b in range(batch)]
    sines = [row_of(sine, b) for b in range(batch)]

    def rotated(rows, cosine, sine):
        return rows * cosine + pltpu.roll(rows, HEAD_SIZE // 2, 1) * sine

    spot = lax.broadcasted_iota(jnp.int32, (group, positions), 1) + me * positions
    masks = [jnp.where(spot < lens_ref[b], 0.0, -1e30) for b in range(batch)]
    units = [(g, b) for g in range(KEY_VALUE_HEADS) for b in range(batch)]

    def stacked(rows):
        return jnp.concatenate(rows, axis=0)

    valid = stacked([masks[b] for g, b in units]) == 0.0
    tokens = KEY_VALUE_HEADS * batch
    first = QUERY_HEADS * batch
    fresh_k = rotated(
        heads[first : first + tokens, :],
        jnp.tile(cosine, (tokens // 8, 1)),
        jnp.tile(sine, (tokens // 8, 1)),
    )
    fresh_v = heads[first + tokens : first + 2 * tokens, :]
    queries, scores = [], []
    for g, b in units:
        q = heads[pl.ds(g * group * batch + b, group, stride=batch), :]
        q = rotated(q, cosines[b], sines[b]).astype(bf16)
        k_rows = kv[b, :, g * HEAD_SIZE : (g + 1) * HEAD_SIZE]
        queries.append(q)
        scores.append(
            lax.dot_general(q, k_rows, (((1,), (1,)), ((), ())), preferred_element_type=f32)
        )
    s = stacked(scores) * inv
    top = jnp.max(jnp.where(valid, s, -1e30), axis=-1, keepdims=True)
    w = jnp.where(valid, jnp.exp(s - top), 0.0)
    total = jnp.sum(w, axis=-1, keepdims=True)
    w = w.astype(bf16)
    o = stacked(
        [
            jnp.dot(
                w[i * group : (i + 1) * group, :],
                vv[b, :, g * HEAD_SIZE : (g + 1) * HEAD_SIZE],
                preferred_element_type=f32,
            )
            for i, (g, b) in enumerate(units)
        ]
    )
    k_new = stacked([row_of(fresh_k, g * batch + b) for g, b in units])
    v_new = stacked([row_of(fresh_v, g * batch + b) for g, b in units])
    s_new = jnp.sum(stacked(queries).astype(f32) * k_new, axis=-1, keepdims=True) * inv
    s_new = jnp.where(me == 0, s_new, -1e30)
    top_new = jnp.maximum(top, s_new)
    keep = jnp.exp(top - top_new)
    fresh = jnp.where(me == 0, jnp.exp(s_new - top_new), 0.0)
    total = total * keep + fresh
    o = o * keep + fresh * v_new
    some = total > 0.0
    safe = jnp.where(some, total, 1.0)
    o = o / safe
    lse = jnp.where(some, top_new + jnp.log(safe), -1e30)
    lse = jnp.broadcast_to(lse, o.shape)
    for i, (g, b) in enumerate(units):
        spread = pl.ds(g * group * batch + b, group, stride=batch)
        ordered[0, spread, :] = o[i * group : (i + 1) * group, :]
        ordered[1, spread, :] = lse[i * group : (i + 1) * group, :]
    own_lane = lax.broadcasted_iota(jnp.int32, (own_rows, LANES), 1)
    own_row = lax.broadcasted_iota(jnp.int32, (own_rows, LANES), 0)
    diagonal = own_lane == own_row
    for e in range(n):
        rows = slice(e * own_rows, (e + 1) * own_rows)
        so[e] = ordered[0, rows, :].astype(bf16)
        sl[e] = jnp.sum(jnp.where(diagonal, ordered[1, rows, :], 0.0), axis=0, keepdims=True)

    def send_o(k, peer):
        remote(so.at[peer], og.at[me], o_send, o_recv, peer).start()
        remote(sl.at[peer], lg.at[me], l_send, l_recv, peer).start()

    far_first(send_o)
    og[me] = so[me]
    lg[me] = sl[me]
    for i in range(groups):
        wo_copy(i).wait()

    all_received(lg, l_send, l_recv)
    all_received(og, o_send, o_recv)

    lses = [
        jnp.sum(jnp.where(diagonal, lg[s], 0.0), axis=-1, keepdims=True) for s in range(n)
    ]
    best = functools.reduce(jnp.maximum, lses)
    den = jnp.zeros_like(best)
    num = jnp.zeros((own_rows, LANES), f32)
    for s in range(n):
        share = jnp.exp(lses[s] - best)
        den = den + share
        num = num + share * og[s].astype(f32)
    att = num / den
    att = jnp.concatenate(
        [att[j * batch : (j + 1) * batch, :] for j in range(own_heads)], axis=1
    ).astype(bf16)

    def rows_of(part):
        return jnp.concatenate(
            [part[:, j * LANES : (j + 1) * LANES] for j in range(pieces)], axis=0
        )

    def send_part(peer, part):
        rs_send[peer] = rows_of(part).astype(bf16)
        remote(rs_send.at[peer], rs_recv.at[me], r_send, r_recv, peer).start()

    def out_of(peer, count):
        span = pl.ds(pl.multiple_of(peer * dx, dx), count * dx)
        return jnp.dot(att, wo[:, span], preferred_element_type=f32)

    def project_out(j, carry):
        first = base_of(groups - 1 - j)
        part = out_of(first, per)
        for u in range(per):
            send_part(first + u, part[:, u * dx : (u + 1) * dx])
        return carry

    lax.fori_loop(0, groups - 2, project_out, 0)
    near = [(base_of(1), per), (half_of(1) // dx, half)]
    parts = [(first, count, out_of(first, count)) for first, count in near]
    for first, count, part in parts:
        for u in range(count):
            send_part(first + u, part[:, u * dx : (u + 1) * dx])
    mate = partner(me, 1, n)
    part, own = out_of(mate, 1), rows_of(out_of(me, 1))
    send_part(mate, part)

    all_received(rs_recv, r_send, r_recv)
    total = own
    if unrolled:
        for k in range(1, n):
            total = total + rs_recv[partner(me, k, n)].astype(f32)
    else:
        total = lax.fori_loop(
            1, n, lambda k, t: t + rs_recv[partner(me, k, n)].astype(f32), total
        )
    out_ref[...] = total.astype(bf16)

    all_sent(stats, t_send, t_recv)
    all_sent(xg, x_send, x_recv.at[0])
    all_sent(qg, q_send, q_recv)
    all_sent(so, o_send, o_recv)
    all_sent(sl, l_send, l_recv)
    all_sent(rs_send, r_send, r_recv)


def hand_over(result_ref, scale_ref, out_ref, token_scale_ref):
    out_ref[...] = result_ref[...]
    token_scale_ref[...] = scale_ref[...]


def on_device(n, hidden_in, norm_gain, w_qkv, w_out, key_cache, value_cache, lengths, positions):
    batch, dx = hidden_in.shape
    cw = w_qkv.shape[1]
    own_rows = w_out.shape[0] // HEAD_SIZE * batch
    total_heads = QUERY_HEADS + 2 * KEY_VALUE_HEADS
    widest = max(d * cw % LANES for d in range(n)) + cw
    blocks = rounded_up(widest, LANES) // LANES
    pieces = dx // LANES
    x_height = rounded_up(pieces * batch, 8) + rounded_up(pieces, 8)
    half = HEAD_SIZE // 2
    freq = np.float32(500000.0) ** (
        -(np.arange(half, dtype=np.float32) * np.float32(2.0)) / np.float32(HEAD_SIZE)
    )
    freq = jnp.asarray(np.tile(freq.astype(np.float32), 2)[None, :])
    bf16, f32 = jnp.bfloat16, jnp.float32
    dma = pltpu.SemaphoreType.DMA
    hbm = pl.BlockSpec(memory_space=pl.ANY)
    vmem = pl.BlockSpec(memory_space=pltpu.VMEM)
    out, token_scale = pl.pallas_call(
        functools.partial(kernel, n),
        out_shape=(
            pltpu.VMEM((pieces * batch, LANES), bf16),
            pltpu.VMEM((1, batch), f32),
        ),
        in_specs=[hbm] * 9,
        out_specs=(vmem, vmem),
        scratch_shapes=[
            pltpu.VMEM((n, x_height, LANES), bf16),
            pltpu.VMEM((n // 2, batch, 2 * dx), bf16),
            pltpu.VMEM((cw, n * dx), bf16),
            pltpu.VMEM(((n - 4) * dx, cw // LANES * LANES), bf16),
            pltpu.VMEM((4 * dx, cw // LANES * LANES), bf16),
            pltpu.VMEM((w_out.shape[0], n * dx), bf16),
            pltpu.VMEM(key_cache.shape, bf16),
            pltpu.VMEM(value_cache.shape, bf16),
            pltpu.VMEM((n, 1, LANES), f32),
            pltpu.VMEM((n, batch, blocks * LANES), bf16),
            pltpu.VMEM((total_heads * batch, HEAD_SIZE), f32),
            pltpu.VMEM((2, QUERY_HEADS * batch, HEAD_SIZE), f32),
            pltpu.VMEM((n, own_rows, LANES), bf16),
            pltpu.VMEM((n, own_rows, LANES), bf16),
            pltpu.VMEM((n, 1, LANES), f32),
            pltpu.VMEM((n, 1, LANES), f32),
            pltpu.VMEM((n, pieces * batch, LANES), bf16),
            pltpu.VMEM((n, pieces * batch, LANES), bf16),
            pltpu.SMEM((batch,), jnp.int32),
            pltpu.SMEM((batch,), jnp.int32),
            pltpu.VMEM((1, LANES), f32),
            dma((5,)),
            dma((n // 2,)),
            dma((n // 4,)),
            dma((2,)),
            dma(()),
            dma(()),
            dma(()),
            dma((n // 4,)),
        ]
        + [dma(())] * 8,
        compiler_params=pltpu.CompilerParams(
            collective_id=0, has_side_effects=True, vmem_limit_bytes=60 * 1024 * 1024
        ),
        name="decode",
    )(
        hidden_in.reshape(batch, pieces, LANES).transpose(1, 0, 2).reshape(-1, LANES),
        norm_gain.reshape(dx // LANES, LANES),
        w_qkv.T,
        w_out,
        key_cache,
        value_cache,
        lengths,
        positions,
        freq,
    )
    out = pltpu.with_memory_space_constraint(out, pltpu.VMEM)
    token_scale = pltpu.with_memory_space_constraint(token_scale, pltpu.VMEM)
    out, token_scale = pl.pallas_call(
        hand_over,
        out_shape=(
            jax.ShapeDtypeStruct(out.shape, out.dtype),
            jax.ShapeDtypeStruct(token_scale.shape, token_scale.dtype),
        ),
        in_specs=[vmem, vmem],
        out_specs=(vmem, vmem),
        name="hand_over",
    )(out, token_scale)
    out = out.reshape(pieces, batch, LANES).transpose(1, 0, 2).reshape(batch, dx)
    return out, token_scale.reshape(batch)


def solution(mesh):
    placed = (
        P("replica", "tp"),
        P("tp"),
        P(None, "tp"),
        P("tp", None),
        P("replica", "tp", None),
        P("replica", "tp", None),
        P("replica"),
        P("replica"),
    )
    return jax.shard_map(
        functools.partial(on_device, mesh.shape["tp"]),
        mesh=mesh,
        in_specs=placed,
        out_specs=(P("replica", "tp"), P("replica")),
        check_vma=False,
    )
```

```python
import functools

import jax
import jax.numpy as jnp
import numpy as np
from jax import lax
from jax.experimental import pallas as pl
from jax.experimental.pallas import tpu as pltpu
from jax.sharding import PartitionSpec as P

QUERY_HEADS = 64
KEY_VALUE_HEADS = 4
HEAD_SIZE = 128
LANES = 128


def rounded_up(value, step):
    return (value + step - 1) // step * step


def partner(me, k, n):
    peer = me
    bit = 1
    while bit < n:
        if isinstance(k, int):
            if k & bit:
                peer = peer + (bit - 2 * bit * ((me // bit) % 2))
        else:
            mine, flip = (me // bit) % 2, (k // bit) % 2
            peer = peer + bit * flip * (1 - 2 * mine)
        bit *= 2
    return peer


def kernel(
    n,
    hidden_hbm,
    gain_hbm,
    wq_hbm,
    wo_hbm,
    key_hbm,
    value_hbm,
    lens_hbm,
    pos_hbm,
    freq_hbm,
    out_ref,
    scale_ref,
    xg,
    quant,
    wq,
    wt,
    wz,
    wo,
    kv,
    vv,
    stats,
    qg,
    heads,
    ordered,
    so,
    og,
    sl,
    lg,
    rs_send,
    rs_recv,
    lens_ref,
    pos_ref,
    freq_ref,
    local_sem,
    wq_sem,
    wo_sem,
    kv_sem,
    t_send,
    t_recv,
    x_send,
    x_recv,
    q_send,
    q_recv,
    o_send,
    o_recv,
    l_send,
    l_recv,
    r_send,
    r_recv,
):
    me = lax.axis_index("tp")
    dx = wo.shape[1] // n
    batch = lens_ref.shape[0]
    pieces = dx // LANES
    x_rows = pieces * batch
    gain_at = xg.shape[1] - rounded_up(pieces, 8)
    cw, width = wq_hbm.shape
    padded = qg.shape[2]
    own_rows = og.shape[1]
    own_heads = own_rows // batch
    positions = key_hbm.shape[1]
    group = QUERY_HEADS // KEY_VALUE_HEADS
    f32, bf16 = jnp.float32, jnp.bfloat16
    unrolled = n <= 16

    per = 4
    groups = n // per
    span_of = lambda base: pl.ds(pl.multiple_of(base * dx, per * dx), per * dx)

    def base_of(i):
        return partner(me, i * per, n) // per * per

    half = per // 2
    turned = wt.shape[1]

    def half_of(i):
        return pl.multiple_of(partner(me, i * half, n) // half * half * dx, half * dx)

    def wq_copy(i):
        span = pl.ds(half_of(i), half * dx)
        return pltpu.make_async_copy(wq_hbm.at[:, span], wq.at[:, span], wq_sem.at[i])

    def turn_into(ref, i, place):
        start = half_of(i)
        for j in range(half * dx // LANES):
            at = pl.multiple_of(start + j * LANES, LANES)
            to = pl.multiple_of(place * half * dx + j * LANES, LANES)
            ref[pl.ds(to, LANES), :] = wq[0:turned, pl.ds(at, LANES)].T

    def turn(i, carry):
        wq_copy(i).wait()
        turn_into(wt, i, i)
        return carry

    def wo_copy(i):
        span = span_of(base_of(i))
        return pltpu.make_async_copy(wo_hbm.at[:, span], wo.at[:, span], wo_sem.at[i])

    def remote(src, dst, send, recv, peer):
        return pltpu.make_async_remote_copy(
            src_ref=src,
            dst_ref=dst,
            send_sem=send,
            recv_sem=recv,
            device_id={"tp": peer},
            device_id_type=pl.DeviceIdType.MESH,
        )

    def far_group(j):
        if groups != 4:
            return groups - 1 - j
        middle = (me // per + me // (2 * per)) % 2
        return [3 - middle, 2 + middle, 1, 0][j]

    def far_first(act):
        if unrolled and groups == 4:
            for j in range(groups):
                for u in range(per - 1, -1, -1):
                    if j == groups - 1 and u == 0:
                        continue
                    k = far_group(j) * per + u
                    act(k, partner(me, k, n))
        elif unrolled:
            for k in range(n - 1, 0, -1):
                act(k, partner(me, k, n))
        else:

            def step(i, carry):
                act(n - 1 - i, partner(me, n - 1 - i, n))
                return carry

            lax.fori_loop(0, n - 1, step, 0)

    def near_first(act):
        if unrolled:
            for k in range(1, n):
                act(k, partner(me, k, n))
        else:

            def step(k, carry):
                act(k, partner(me, k, n))
                return carry

            lax.fori_loop(1, n, step, 0)

    def all_sent(ref, send, recv):
        part = ref.at[pl.ds(0, n - 1)]
        remote(part, part, send, recv, partner(me, 1, n)).wait_send()

    def all_received(ref, send, recv, count=n - 1):
        part = ref.at[pl.ds(0, count)]
        remote(part, part, send, recv, partner(me, 1, n)).wait_recv()

    small = [
        (hidden_hbm, xg.at[me, pl.ds(0, x_rows), :]),
        (gain_hbm, xg.at[me, pl.ds(gain_at, pieces), :]),
        (freq_hbm, freq_ref),
        (pos_hbm, pos_ref),
        (lens_hbm, lens_ref),
    ]
    small = [
        pltpu.make_async_copy(src, dst, local_sem.at[i]) for i, (src, dst) in enumerate(small)
    ]
    for copy in small:
        copy.start()

    barrier = pltpu.get_barrier_semaphore()
    def announce(peer):
        pl.semaphore_signal(
            barrier, inc=1, device_id={"tp": peer}, device_id_type=pl.DeviceIdType.MESH
        )

    if unrolled:
        for k in range(n - 1, 0, -1):
            announce(partner(me, k, n))
    else:
        far_first(lambda k, peer: announce(peer))
    copy_k = pltpu.make_async_copy(key_hbm, kv, kv_sem.at[0])
    copy_v = pltpu.make_async_copy(value_hbm, vv, kv_sem.at[1])

    small[0].wait()
    small[1].wait()

    half8 = lax.broadcasted_iota(jnp.int32, (8, LANES), 0) // batch
    row4 = lax.broadcasted_iota(jnp.int32, (8, LANES), 0) % batch
    lane8 = lax.broadcasted_iota(jnp.int32, (8, LANES), 1)
    per8 = 8 // batch

    def gained(s):
        x = xg[s, 0:x_rows, :].astype(f32)
        g = xg[s, gain_at : gain_at + rounded_up(pieces, 8), :].astype(f32)
        xs, ys = [], []
        for j in range(x_rows // 8):
            x8 = x[8 * j : 8 * j + 8, :]
            g8 = jnp.zeros((8, LANES), f32)
            for u in range(per8):
                r = j * per8 + u
                g8 = jnp.where(half8 == u, g[r : r + 1, :], g8)
            xs.append(x8)
            ys.append(x8 * g8)
        return xs, ys

    xs, ys = gained(me)
    squares = sum(x8 * x8 for x8 in xs)
    peak = functools.reduce(jnp.maximum, [jnp.abs(y) for y in ys])
    squares = jnp.sum(squares, axis=-1, keepdims=True)
    peak = jnp.max(peak, axis=-1, keepdims=True)
    first = jnp.sum(jnp.where(lane8 == row4, squares, 0.0), axis=0, keepdims=True)
    second = jnp.max(jnp.where(lane8 == row4 + batch, peak, 0.0), axis=0, keepdims=True)
    stats[me] = jnp.where(lane8[0:1, :] < batch, first, second)

    for i in range(2 * groups):
        wq_copy(i).start()

    pl.semaphore_wait(barrier, n - 1)

    far_first(
        lambda k, peer: remote(stats.at[me], stats.at[me], t_send, t_recv, peer).start()
    )
    def send_x(k, peer):
        remote(xg.at[me], xg.at[me], x_send, x_recv.at[k // per], peer).start()

    near_first(send_x)

    for copy in small[2:]:
        copy.wait()
    place = jnp.zeros((8, LANES), f32)
    for b in range(batch):
        place = jnp.where(row4 == b, pos_ref[b].astype(f32), place)
    angle = place * freq_ref[...]
    cosine = jnp.cos(angle)
    sine = jnp.sin(angle)
    sine = jnp.where(lane8 < HEAD_SIZE // 2, -sine, sine)

    lax.fori_loop(0, 2 * groups - 2, turn, 0)
    all_received(stats, t_send, t_recv)
    if n % 8 == 0:
        rows = [stats[8 * i : 8 * i + 8, 0, :] for i in range(n // 8)]
        added = jnp.sum(sum(rows), axis=0, keepdims=True)
        largest = jnp.max(functools.reduce(jnp.maximum, rows), axis=0, keepdims=True)
    else:
        rows = [stats[i] for i in range(n)]
        added = sum(rows)
        largest = functools.reduce(jnp.maximum, rows)
    added = jnp.sum(jnp.where(lane8 == row4, added, 0.0), axis=-1, keepdims=True)
    largest = jnp.max(jnp.where(lane8 == row4 + batch, largest, 0.0), axis=-1, keepdims=True)
    rstd8 = lax.rsqrt(added / width + 1e-05)
    scale8 = (largest * rstd8 + 1e-06) / 448.0
    token_scale = scale8[0:batch, :]
    scale_ref[...] = jnp.sum(
        jnp.where((lane8 == row4) & (half8 == 0), scale8, 0.0), axis=0, keepdims=True
    )[:, 0:batch]
    rstd8 = jnp.broadcast_to(rstd8, (8, LANES))
    scale8 = jnp.broadcast_to(scale8, (8, LANES))

    copy_k.start()
    copy_v.start()
    for i in range(groups - 1, -1, -1):
        wo_copy(i).start()

    def project(i, carry, ref, place):
        acc, rest = carry
        for v in range(2):
            first = half_of(2 * i + v) // dx
            for u in range(half):
                _, ys = gained(first + u)
                rows = [y * rstd8 / scale8 for y in ys]
                flat = [row[w * batch : (w + 1) * batch, :] for row in rows for w in range(per8)]
                quant[2 * i + v, :, u * dx : (u + 1) * dx] = jnp.concatenate(
                    flat, axis=1
                ).astype(bf16)
        for v in range(2):
            x = quant[2 * i + v]
            to = pl.multiple_of((2 * place + v) * half * dx, half * dx)
            acc = acc + jnp.dot(x, ref[pl.ds(to, half * dx), :], preferred_element_type=f32)
            if turned < cw:
                rest = rest + lax.dot_general(
                    wq[turned:cw, pl.ds(half_of(2 * i + v), half * dx)],
                    x,
                    (((1,), (1,)), ((), ())),
                    preferred_element_type=f32,
                )
        return acc, rest

    def project_middle(i, carry):
        all_received(xg, x_send, x_recv.at[i], per)
        return project(i, carry, wt, i)

    carry = (jnp.zeros((batch, turned), f32), jnp.zeros((cw - turned, batch), f32))
    for i in range(2):
        wq_copy(2 * groups - 2 + i).wait()
        all_received(xg, x_send, x_recv.at[i], per if i else per - 1)
        turn_into(wz, 2 * groups - 2 + i, i)
        carry = project(i, carry, wt, i)
    carry = lax.fori_loop(2, groups - 1, project_middle, carry)
    all_received(xg, x_send, x_recv.at[groups - 1], per)
    acc, rest = project(groups - 1, carry, wz, 0)
    if turned < cw:
        acc = jnp.concatenate([acc, rest.T], axis=1)
    proj = (acc * token_scale).astype(bf16).astype(f32)
    if padded > cw:
        proj = jnp.concatenate([proj, jnp.zeros((batch, padded - cw), f32)], axis=1)
    if cw % LANES:
        proj = pltpu.roll(proj, lax.rem(me * cw, LANES), 1)
    qg[me] = proj.astype(bf16)
    far_first(lambda k, peer: remote(qg.at[me], qg.at[me], q_send, q_recv, peer).start())
    copy_k.wait()
    copy_v.wait()
    all_received(qg, q_send, q_recv)

    total_heads = QUERY_HEADS + 2 * KEY_VALUE_HEADS
    unpacked = [qg[d].astype(f32) for d in range(n)]
    for h in range(total_heads):
        piece = None
        for d in range(h * LANES // cw, (h * LANES + LANES - 1) // cw + 1):
            block = h - d * cw // LANES
            part = unpacked[d][:, block * LANES : (block + 1) * LANES]
            piece = part if piece is None else piece + part
        heads[h * batch : (h + 1) * batch, :] = piece

    inv = 1.0 / HEAD_SIZE**0.5

    def row_of(rows, b):
        return jnp.broadcast_to(rows[b : b + 1, :], (group, HEAD_SIZE))

    cosines = [row_of(cosine, b) for b in range(batch)]
    sines = [row_of(sine, b) for b in range(batch)]

    def rotated(rows, cosine, sine):
        return rows * cosine + pltpu.roll(rows, HEAD_SIZE // 2, 1) * sine

    spot = lax.broadcasted_iota(jnp.int32, (group, positions), 1) + me * positions
    masks = [jnp.where(spot < lens_ref[b], 0.0, -1e30) for b in range(batch)]
    units = [(g, b) for g in range(KEY_VALUE_HEADS) for b in range(batch)]

    def stacked(rows):
        return jnp.concatenate(rows, axis=0)

    valid = stacked([masks[b] for g, b in units]) == 0.0
    tokens = KEY_VALUE_HEADS * batch
    first = QUERY_HEADS * batch
    fresh_k = rotated(
        heads[first : first + tokens, :],
        jnp.tile(cosine, (tokens // 8, 1)),
        jnp.tile(sine, (tokens // 8, 1)),
    )
    fresh_v = heads[first + tokens : first + 2 * tokens, :]
    queries, scores = [], []
    for g, b in units:
        q = heads[pl.ds(g * group * batch + b, group, stride=batch), :]
        q = rotated(q, cosines[b], sines[b]).astype(bf16)
        k_rows = kv[b, :, g * HEAD_SIZE : (g + 1) * HEAD_SIZE]
        queries.append(q)
        scores.append(
            lax.dot_general(q, k_rows, (((1,), (1,)), ((), ())), preferred_element_type=f32)
        )
    s = stacked(scores) * inv
    top = jnp.max(jnp.where(valid, s, -1e30), axis=-1, keepdims=True)
    w = jnp.where(valid, jnp.exp(s - top), 0.0)
    total = jnp.sum(w, axis=-1, keepdims=True)
    w = w.astype(bf16)
    o = stacked(
        [
            jnp.dot(
                w[i * group : (i + 1) * group, :],
                vv[b, :, g * HEAD_SIZE : (g + 1) * HEAD_SIZE],
                preferred_element_type=f32,
            )
            for i, (g, b) in enumerate(units)
        ]
    )
    k_new = stacked([row_of(fresh_k, g * batch + b) for g, b in units])
    v_new = stacked([row_of(fresh_v, g * batch + b) for g, b in units])
    s_new = jnp.sum(stacked(queries).astype(f32) * k_new, axis=-1, keepdims=True) * inv
    s_new = jnp.where(me == 0, s_new, -1e30)
    top_new = jnp.maximum(top, s_new)
    keep = jnp.exp(top - top_new)
    fresh = jnp.where(me == 0, jnp.exp(s_new - top_new), 0.0)
    total = total * keep + fresh
    o = o * keep + fresh * v_new
    some = total > 0.0
    safe = jnp.where(some, total, 1.0)
    o = o / safe
    lse = jnp.where(some, top_new + jnp.log(safe), -1e30)
    lse = jnp.broadcast_to(lse, o.shape)
    for i, (g, b) in enumerate(units):
        spread = pl.ds(g * group * batch + b, group, stride=batch)
        ordered[0, spread, :] = o[i * group : (i + 1) * group, :]
        ordered[1, spread, :] = lse[i * group : (i + 1) * group, :]
    own_lane = lax.broadcasted_iota(jnp.int32, (own_rows, LANES), 1)
    own_row = lax.broadcasted_iota(jnp.int32, (own_rows, LANES), 0)
    diagonal = own_lane == own_row
    for e in range(n):
        rows = slice(e * own_rows, (e + 1) * own_rows)
        so[e] = ordered[0, rows, :].astype(bf16)
        sl[e] = jnp.sum(jnp.where(diagonal, ordered[1, rows, :], 0.0), axis=0, keepdims=True)

    def send_o(k, peer):
        remote(so.at[peer], og.at[me], o_send, o_recv, peer).start()
        remote(sl.at[peer], lg.at[me], l_send, l_recv, peer).start()

    far_first(send_o)
    og[me] = so[me]
    lg[me] = sl[me]
    for i in range(groups):
        wo_copy(i).wait()

    all_received(lg, l_send, l_recv)
    all_received(og, o_send, o_recv)

    lses = [
        jnp.sum(jnp.where(diagonal, lg[s], 0.0), axis=-1, keepdims=True) for s in range(n)
    ]
    best = functools.reduce(jnp.maximum, lses)
    den = jnp.zeros_like(best)
    num = jnp.zeros((own_rows, LANES), f32)
    for s in range(n):
        share = jnp.exp(lses[s] - best)
        den = den + share
        num = num + share * og[s].astype(f32)
    att = num / den
    att = jnp.concatenate(
        [att[j * batch : (j + 1) * batch, :] for j in range(own_heads)], axis=1
    ).astype(bf16)

    def rows_of(part):
        return jnp.concatenate(
            [part[:, j * LANES : (j + 1) * LANES] for j in range(pieces)], axis=0
        )

    def send_part(peer, part):
        rs_send[peer] = rows_of(part).astype(bf16)
        remote(rs_send.at[peer], rs_recv.at[me], r_send, r_recv, peer).start()

    def out_of(peer, count):
        span = pl.ds(pl.multiple_of(peer * dx, dx), count * dx)
        return jnp.dot(att, wo[:, span], preferred_element_type=f32)

    def project_out(i):
        first = base_of(i)
        part = out_of(first, per)
        for u in range(per):
            send_part(first + u, part[:, u * dx : (u + 1) * dx])

    def project_far(j, carry):
        if groups == 4:
            middle = (me // per + me // (2 * per)) % 2
            project_out(3 - j - middle * (1 - 2 * j))
        else:
            project_out(groups - 1 - j)
        return carry

    lax.fori_loop(0, groups - 2, project_far, 0)
    near = [(base_of(1), per), (half_of(1) // dx, half)]
    parts = [(first, count, out_of(first, count)) for first, count in near]
    for first, count, part in parts:
        for u in range(count):
            send_part(first + u, part[:, u * dx : (u + 1) * dx])
    mate = partner(me, 1, n)
    part, own = out_of(mate, 1), rows_of(out_of(me, 1))
    send_part(mate, part)

    all_received(rs_recv, r_send, r_recv)
    total = own
    if unrolled:
        for k in range(1, n):
            total = total + rs_recv[partner(me, k, n)].astype(f32)
    else:
        total = lax.fori_loop(
            1, n, lambda k, t: t + rs_recv[partner(me, k, n)].astype(f32), total
        )
    out_ref[...] = total.astype(bf16)

    all_sent(stats, t_send, t_recv)
    all_sent(xg, x_send, x_recv.at[0])
    all_sent(qg, q_send, q_recv)
    all_sent(so, o_send, o_recv)
    all_sent(sl, l_send, l_recv)
    all_sent(rs_send, r_send, r_recv)


def hand_over(result_ref, scale_ref, out_ref, token_scale_ref):
    out_ref[...] = result_ref[...]
    token_scale_ref[...] = scale_ref[...]


def on_device(n, hidden_in, norm_gain, w_qkv, w_out, key_cache, value_cache, lengths, positions):
    batch, dx = hidden_in.shape
    cw = w_qkv.shape[1]
    own_rows = w_out.shape[0] // HEAD_SIZE * batch
    total_heads = QUERY_HEADS + 2 * KEY_VALUE_HEADS
    widest = max(d * cw % LANES for d in range(n)) + cw
    blocks = rounded_up(widest, LANES) // LANES
    pieces = dx // LANES
    x_height = rounded_up(pieces * batch, 8) + rounded_up(pieces, 8)
    half = HEAD_SIZE // 2
    freq = np.float32(500000.0) ** (
        -(np.arange(half, dtype=np.float32) * np.float32(2.0)) / np.float32(HEAD_SIZE)
    )
    freq = jnp.asarray(np.tile(freq.astype(np.float32), 2)[None, :])
    bf16, f32 = jnp.bfloat16, jnp.float32
    dma = pltpu.SemaphoreType.DMA
    hbm = pl.BlockSpec(memory_space=pl.ANY)
    vmem = pl.BlockSpec(memory_space=pltpu.VMEM)
    out, token_scale = pl.pallas_call(
        functools.partial(kernel, n),
        out_shape=(
            pltpu.VMEM((pieces * batch, LANES), bf16),
            pltpu.VMEM((1, batch), f32),
        ),
        in_specs=[hbm] * 9,
        out_specs=(vmem, vmem),
        scratch_shapes=[
            pltpu.VMEM((n, x_height, LANES), bf16),
            pltpu.VMEM((n // 2, batch, 2 * dx), bf16),
            pltpu.VMEM((cw, n * dx), bf16),
            pltpu.VMEM(((n - 4) * dx, cw // LANES * LANES), bf16),
            pltpu.VMEM((4 * dx, cw // LANES * LANES), bf16),
            pltpu.VMEM((w_out.shape[0], n * dx), bf16),
            pltpu.VMEM(key_cache.shape, bf16),
            pltpu.VMEM(value_cache.shape, bf16),
            pltpu.VMEM((n, 1, LANES), f32),
            pltpu.VMEM((n, batch, blocks * LANES), bf16),
            pltpu.VMEM((total_heads * batch, HEAD_SIZE), f32),
            pltpu.VMEM((2, QUERY_HEADS * batch, HEAD_SIZE), f32),
            pltpu.VMEM((n, own_rows, LANES), bf16),
            pltpu.VMEM((n, own_rows, LANES), bf16),
            pltpu.VMEM((n, 1, LANES), f32),
            pltpu.VMEM((n, 1, LANES), f32),
            pltpu.VMEM((n, pieces * batch, LANES), bf16),
            pltpu.VMEM((n, pieces * batch, LANES), bf16),
            pltpu.SMEM((batch,), jnp.int32),
            pltpu.SMEM((batch,), jnp.int32),
            pltpu.VMEM((1, LANES), f32),
            dma((5,)),
            dma((n // 2,)),
            dma((n // 4,)),
            dma((2,)),
            dma(()),
            dma(()),
            dma(()),
            dma((n // 4,)),
        ]
        + [dma(())] * 8,
        compiler_params=pltpu.CompilerParams(
            collective_id=0, has_side_effects=True, vmem_limit_bytes=60 * 1024 * 1024
        ),
        name="decode",
    )(
        hidden_in.reshape(batch, pieces, LANES).transpose(1, 0, 2).reshape(-1, LANES),
        norm_gain.reshape(dx // LANES, LANES),
        w_qkv.T,
        w_out,
        key_cache,
        value_cache,
        lengths,
        positions,
        freq,
    )
    out = pltpu.with_memory_space_constraint(out, pltpu.VMEM)
    token_scale = pltpu.with_memory_space_constraint(token_scale, pltpu.VMEM)
    out, token_scale = pl.pallas_call(
        hand_over,
        out_shape=(
            jax.ShapeDtypeStruct(out.shape, out.dtype),
            jax.ShapeDtypeStruct(token_scale.shape, token_scale.dtype),
        ),
        in_specs=[vmem, vmem],
        out_specs=(vmem, vmem),
        name="hand_over",
    )(out, token_scale)
    out = out.reshape(pieces, batch, LANES).transpose(1, 0, 2).reshape(batch, dx)
    return out, token_scale.reshape(batch)


def solution(mesh):
    placed = (
        P("replica", "tp"),
        P("tp"),
        P(None, "tp"),
        P("tp", None),
        P("replica", "tp", None),
        P("replica", "tp", None),
        P("replica"),
        P("replica"),
    )
    return jax.shard_map(
        functools.partial(on_device, mesh.shape["tp"]),
        mesh=mesh,
        in_specs=placed,
        out_specs=(P("replica", "tp"), P("replica")),
        check_vma=False,
    )
```

```python
import functools

import jax
import jax.numpy as jnp
import numpy as np
from jax import lax
from jax.experimental import pallas as pl
from jax.experimental.pallas import tpu as pltpu
from jax.sharding import PartitionSpec as P

QUERY_HEADS = 64
KEY_VALUE_HEADS = 4
HEAD_SIZE = 128
LANES = 128


def rounded_up(value, step):
    return (value + step - 1) // step * step


def partner(me, k, n):
    peer = me
    bit = 1
    while bit < n:
        if isinstance(k, int):
            if k & bit:
                peer = peer + (bit - 2 * bit * ((me // bit) % 2))
        else:
            mine, flip = (me // bit) % 2, (k // bit) % 2
            peer = peer + bit * flip * (1 - 2 * mine)
        bit *= 2
    return peer


def kernel(
    n,
    hidden_hbm,
    gain_hbm,
    wq_hbm,
    wo_hbm,
    key_hbm,
    value_hbm,
    lens_hbm,
    pos_hbm,
    freq_hbm,
    out_ref,
    scale_ref,
    xg,
    quant,
    wq,
    wt,
    wz,
    wo,
    kv,
    kt,
    vv,
    stats,
    qg,
    heads,
    ordered,
    so,
    og,
    sl,
    lg,
    rs_send,
    rs_recv,
    lens_ref,
    pos_ref,
    freq_ref,
    local_sem,
    wq_sem,
    wo_sem,
    kv_sem,
    t_send,
    t_recv,
    x_send,
    x_recv,
    q_send,
    q_recv,
    o_send,
    o_recv,
    l_send,
    l_recv,
    r_send,
    r_recv,
):
    me = lax.axis_index("tp")
    dx = wo.shape[1] // n
    batch = lens_ref.shape[0]
    pieces = dx // LANES
    x_rows = pieces * batch
    gain_at = xg.shape[1] - rounded_up(pieces, 8)
    cw, width = wq_hbm.shape
    padded = qg.shape[2]
    own_rows = og.shape[1]
    own_heads = own_rows // batch
    positions = key_hbm.shape[1]
    group = QUERY_HEADS // KEY_VALUE_HEADS
    f32, bf16 = jnp.float32, jnp.bfloat16
    unrolled = n <= 16

    per = 4
    groups = n // per
    span_of = lambda base: pl.ds(pl.multiple_of(base * dx, per * dx), per * dx)

    def base_of(i):
        return partner(me, i * per, n) // per * per

    half = per // 2
    turned = wt.shape[1]

    def half_of(i):
        return pl.multiple_of(partner(me, i * half, n) // half * half * dx, half * dx)

    def wq_copy(i):
        span = pl.ds(half_of(i), half * dx)
        return pltpu.make_async_copy(wq_hbm.at[:, span], wq.at[:, span], wq_sem.at[i])

    def turn_into(ref, i, place):
        start = half_of(i)
        for j in range(half * dx // LANES):
            at = pl.multiple_of(start + j * LANES, LANES)
            to = pl.multiple_of(place * half * dx + j * LANES, LANES)
            ref[pl.ds(to, LANES), :] = wq[0:turned, pl.ds(at, LANES)].T

    def turn(i, carry):
        wq_copy(i).wait()
        turn_into(wt, i, i)
        return carry

    def wo_copy(i):
        span = span_of(base_of(i))
        return pltpu.make_async_copy(wo_hbm.at[:, span], wo.at[:, span], wo_sem.at[i])

    def remote(src, dst, send, recv, peer):
        return pltpu.make_async_remote_copy(
            src_ref=src,
            dst_ref=dst,
            send_sem=send,
            recv_sem=recv,
            device_id={"tp": peer},
            device_id_type=pl.DeviceIdType.MESH,
        )

    def far_group(j):
        if groups != 4:
            return groups - 1 - j
        middle = (me // per + me // (2 * per)) % 2
        return [3 - middle, 2 + middle, 1, 0][j]

    def far_first(act):
        if unrolled and groups == 4:
            for j in range(groups):
                for u in range(per - 1, -1, -1):
                    if j == groups - 1 and u == 0:
                        continue
                    k = far_group(j) * per + u
                    act(k, partner(me, k, n))
        elif unrolled:
            for k in range(n - 1, 0, -1):
                act(k, partner(me, k, n))
        else:

            def step(i, carry):
                act(n - 1 - i, partner(me, n - 1 - i, n))
                return carry

            lax.fori_loop(0, n - 1, step, 0)

    def near_first(act):
        if unrolled:
            for k in range(1, n):
                act(k, partner(me, k, n))
        else:

            def step(k, carry):
                act(k, partner(me, k, n))
                return carry

            lax.fori_loop(1, n, step, 0)

    def all_sent(ref, send, recv):
        part = ref.at[pl.ds(0, n - 1)]
        remote(part, part, send, recv, partner(me, 1, n)).wait_send()

    def all_received(ref, send, recv, count=n - 1):
        part = ref.at[pl.ds(0, count)]
        remote(part, part, send, recv, partner(me, 1, n)).wait_recv()

    small = [
        (hidden_hbm, xg.at[me, pl.ds(0, x_rows), :]),
        (gain_hbm, xg.at[me, pl.ds(gain_at, pieces), :]),
        (freq_hbm, freq_ref),
        (pos_hbm, pos_ref),
        (lens_hbm, lens_ref),
    ]
    small = [
        pltpu.make_async_copy(src, dst, local_sem.at[i]) for i, (src, dst) in enumerate(small)
    ]
    for copy in small:
        copy.start()

    barrier = pltpu.get_barrier_semaphore()
    def announce(peer):
        pl.semaphore_signal(
            barrier, inc=1, device_id={"tp": peer}, device_id_type=pl.DeviceIdType.MESH
        )

    if unrolled:
        for k in range(n - 1, 0, -1):
            announce(partner(me, k, n))
    else:
        far_first(lambda k, peer: announce(peer))
    copy_k = pltpu.make_async_copy(key_hbm, kv, kv_sem.at[0])
    copy_v = pltpu.make_async_copy(value_hbm, vv, kv_sem.at[1])

    for i in range(2 * groups):
        wq_copy(i).start()
    small[0].wait()
    small[1].wait()

    half8 = lax.broadcasted_iota(jnp.int32, (8, LANES), 0) // batch
    row4 = lax.broadcasted_iota(jnp.int32, (8, LANES), 0) % batch
    lane8 = lax.broadcasted_iota(jnp.int32, (8, LANES), 1)
    per8 = 8 // batch

    def gained(s):
        x = xg[s, 0:x_rows, :].astype(f32)
        g = xg[s, gain_at : gain_at + rounded_up(pieces, 8), :].astype(f32)
        xs, ys = [], []
        for j in range(x_rows // 8):
            x8 = x[8 * j : 8 * j + 8, :]
            g8 = jnp.zeros((8, LANES), f32)
            for u in range(per8):
                r = j * per8 + u
                g8 = jnp.where(half8 == u, g[r : r + 1, :], g8)
            xs.append(x8)
            ys.append(x8 * g8)
        return xs, ys

    xs, ys = gained(me)
    squares = sum(x8 * x8 for x8 in xs)
    peak = functools.reduce(jnp.maximum, [jnp.abs(y) for y in ys])
    squares = jnp.sum(squares, axis=-1, keepdims=True)
    peak = jnp.max(peak, axis=-1, keepdims=True)
    first = jnp.sum(jnp.where(lane8 == row4, squares, 0.0), axis=0, keepdims=True)
    second = jnp.max(jnp.where(lane8 == row4 + batch, peak, 0.0), axis=0, keepdims=True)
    stats[me] = jnp.where(lane8[0:1, :] < batch, first, second)


    pl.semaphore_wait(barrier, n - 1)

    far_first(
        lambda k, peer: remote(stats.at[me], stats.at[me], t_send, t_recv, peer).start()
    )
    def send_x(k, peer):
        remote(xg.at[me], xg.at[me], x_send, x_recv.at[k // per], peer).start()

    near_first(send_x)

    lax.fori_loop(0, 2 * groups - 2, turn, 0)
    all_received(stats, t_send, t_recv)
    if n % 8 == 0:
        rows = [stats[8 * i : 8 * i + 8, 0, :] for i in range(n // 8)]
        added = jnp.sum(sum(rows), axis=0, keepdims=True)
        largest = jnp.max(functools.reduce(jnp.maximum, rows), axis=0, keepdims=True)
    else:
        rows = [stats[i] for i in range(n)]
        added = sum(rows)
        largest = functools.reduce(jnp.maximum, rows)
    added = jnp.sum(jnp.where(lane8 == row4, added, 0.0), axis=-1, keepdims=True)
    largest = jnp.max(jnp.where(lane8 == row4 + batch, largest, 0.0), axis=-1, keepdims=True)
    rstd8 = lax.rsqrt(added / width + 1e-05)
    scale8 = (largest * rstd8 + 1e-06) / 448.0
    token_scale = scale8[0:batch, :]
    scale_ref[...] = jnp.sum(
        jnp.where((lane8 == row4) & (half8 == 0), scale8, 0.0), axis=0, keepdims=True
    )[:, 0:batch]
    rstd8 = jnp.broadcast_to(rstd8, (8, LANES))
    scale8 = jnp.broadcast_to(scale8, (8, LANES))

    copy_k.start()
    copy_v.start()
    for i in range(groups - 1, -1, -1):
        wo_copy(i).start()

    def project(i, carry, ref, place):
        acc, rest = carry
        for v in range(2):
            first = half_of(2 * i + v) // dx
            for u in range(half):
                _, ys = gained(first + u)
                rows = [y * rstd8 / scale8 for y in ys]
                flat = [row[w * batch : (w + 1) * batch, :] for row in rows for w in range(per8)]
                quant[2 * i + v, :, u * dx : (u + 1) * dx] = jnp.concatenate(
                    flat, axis=1
                ).astype(bf16)
        for v in range(2):
            x = quant[2 * i + v]
            to = pl.multiple_of((2 * place + v) * half * dx, half * dx)
            acc = acc + jnp.dot(x, ref[pl.ds(to, half * dx), :], preferred_element_type=f32)
            if turned < cw:
                rest = rest + lax.dot_general(
                    x,
                    wq[turned:cw, pl.ds(half_of(2 * i + v), half * dx)],
                    (((1,), (1,)), ((), ())),
                    preferred_element_type=f32,
                )
        return acc, rest

    def project_middle(i, carry):
        all_received(xg, x_send, x_recv.at[i], per)
        return project(i, carry, wt, i)

    carry = (jnp.zeros((batch, turned), f32), jnp.zeros((batch, cw - turned), f32))
    for i in range(2):
        wq_copy(2 * groups - 2 + i).wait()
        all_received(xg, x_send, x_recv.at[i], per if i else per - 1)
        turn_into(wz, 2 * groups - 2 + i, i)
        carry = project(i, carry, wt, i)
    carry = lax.fori_loop(2, groups - 1, project_middle, carry)
    all_received(xg, x_send, x_recv.at[groups - 1], per)
    acc, rest = project(groups - 1, carry, wz, 0)
    if turned < cw:
        acc = jnp.concatenate([acc, rest], axis=1)
    proj = (acc * token_scale).astype(bf16).astype(f32)
    if padded > cw:
        proj = jnp.concatenate([proj, jnp.zeros((batch, padded - cw), f32)], axis=1)
    if cw % LANES:
        proj = pltpu.roll(proj, lax.rem(me * cw, LANES), 1)
    qg[me] = proj.astype(bf16)
    far_first(lambda k, peer: remote(qg.at[me], qg.at[me], q_send, q_recv, peer).start())
    for copy in small[2:]:
        copy.wait()
    place = jnp.zeros((8, LANES), f32)
    for b in range(batch):
        place = jnp.where(row4 == b, pos_ref[b].astype(f32), place)
    angle = place * freq_ref[...]
    cosine = jnp.cos(angle)
    sine = jnp.sin(angle)
    sine = jnp.where(lane8 < HEAD_SIZE // 2, -sine, sine)

    copy_k.wait()
    copy_v.wait()
    for b in range(batch):
        kt[b] = kv[b].T
    all_received(qg, q_send, q_recv)

    total_heads = QUERY_HEADS + 2 * KEY_VALUE_HEADS
    unpacked = [qg[d].astype(f32) for d in range(n)]
    for h in range(total_heads):
        piece = None
        for d in range(h * LANES // cw, (h * LANES + LANES - 1) // cw + 1):
            block = h - d * cw // LANES
            part = unpacked[d][:, block * LANES : (block + 1) * LANES]
            piece = part if piece is None else piece + part
        heads[h * batch : (h + 1) * batch, :] = piece

    inv = 1.0 / HEAD_SIZE**0.5

    def row_of(rows, b):
        return jnp.broadcast_to(rows[b : b + 1, :], (group, HEAD_SIZE))

    cosines = [row_of(cosine, b) for b in range(batch)]
    sines = [row_of(sine, b) for b in range(batch)]

    def rotated(rows, cosine, sine):
        return rows * cosine + pltpu.roll(rows, HEAD_SIZE // 2, 1) * sine

    spot = lax.broadcasted_iota(jnp.int32, (group, positions), 1) + me * positions
    masks = [jnp.where(spot < lens_ref[b], 0.0, -1e30) for b in range(batch)]
    units = [(g, b) for g in range(KEY_VALUE_HEADS) for b in range(batch)]

    def stacked(rows):
        return jnp.concatenate(rows, axis=0)

    valid = stacked([masks[b] for g, b in units]) == 0.0
    tokens = KEY_VALUE_HEADS * batch
    first = QUERY_HEADS * batch
    fresh_k = rotated(
        heads[first : first + tokens, :],
        jnp.tile(cosine, (tokens // 8, 1)),
        jnp.tile(sine, (tokens // 8, 1)),
    )
    fresh_v = heads[first + tokens : first + 2 * tokens, :]
    queries, scores = [], []
    for g, b in units:
        q = heads[pl.ds(g * group * batch + b, group, stride=batch), :]
        q = rotated(q, cosines[b], sines[b]).astype(bf16)
        keys = kt[b, g * HEAD_SIZE : (g + 1) * HEAD_SIZE, :]
        queries.append(q)
        scores.append(jnp.dot(q, keys, preferred_element_type=f32))
    s = stacked(scores) * inv
    top = jnp.max(jnp.where(valid, s, -1e30), axis=-1, keepdims=True)
    w = jnp.where(valid, jnp.exp(s - top), 0.0)
    total = jnp.sum(w, axis=-1, keepdims=True)
    w = w.astype(bf16)
    o = stacked(
        [
            jnp.dot(
                w[i * group : (i + 1) * group, :],
                vv[b, :, g * HEAD_SIZE : (g + 1) * HEAD_SIZE],
                preferred_element_type=f32,
            )
            for i, (g, b) in enumerate(units)
        ]
    )
    k_new = stacked([row_of(fresh_k, g * batch + b) for g, b in units])
    v_new = stacked([row_of(fresh_v, g * batch + b) for g, b in units])
    s_new = jnp.sum(stacked(queries).astype(f32) * k_new, axis=-1, keepdims=True) * inv
    s_new = jnp.where(me == 0, s_new, -1e30)
    top_new = jnp.maximum(top, s_new)
    keep = jnp.exp(top - top_new)
    fresh = jnp.where(me == 0, jnp.exp(s_new - top_new), 0.0)
    total = total * keep + fresh
    o = o * keep + fresh * v_new
    some = total > 0.0
    safe = jnp.where(some, total, 1.0)
    o = o / safe
    lse = jnp.where(some, top_new + jnp.log(safe), -1e30)
    lse = jnp.broadcast_to(lse, o.shape)
    for i, (g, b) in enumerate(units):
        spread = pl.ds(g * group * batch + b, group, stride=batch)
        ordered[0, spread, :] = o[i * group : (i + 1) * group, :]
        ordered[1, spread, :] = lse[i * group : (i + 1) * group, :]
    own_lane = lax.broadcasted_iota(jnp.int32, (own_rows, LANES), 1)
    own_row = lax.broadcasted_iota(jnp.int32, (own_rows, LANES), 0)
    diagonal = own_lane == own_row
    for e in range(n):
        rows = slice(e * own_rows, (e + 1) * own_rows)
        so[e] = ordered[0, rows, :].astype(bf16)
        sl[e] = jnp.sum(jnp.where(diagonal, ordered[1, rows, :], 0.0), axis=0, keepdims=True)

    def send_o(k, peer):
        remote(so.at[peer], og.at[me], o_send, o_recv, peer).start()
        remote(sl.at[peer], lg.at[me], l_send, l_recv, peer).start()

    far_first(send_o)
    og[me] = so[me]
    lg[me] = sl[me]
    for i in range(groups):
        wo_copy(i).wait()

    all_received(lg, l_send, l_recv)
    all_received(og, o_send, o_recv)

    lses = [
        jnp.sum(jnp.where(diagonal, lg[s], 0.0), axis=-1, keepdims=True) for s in range(n)
    ]
    best = functools.reduce(jnp.maximum, lses)
    den = jnp.zeros_like(best)
    num = jnp.zeros((own_rows, LANES), f32)
    for s in range(n):
        share = jnp.exp(lses[s] - best)
        den = den + share
        num = num + share * og[s].astype(f32)
    att = num / den
    att = jnp.concatenate(
        [att[j * batch : (j + 1) * batch, :] for j in range(own_heads)], axis=1
    ).astype(bf16)

    def rows_of(part):
        return jnp.concatenate(
            [part[:, j * LANES : (j + 1) * LANES] for j in range(pieces)], axis=0
        )

    def send_part(peer, part):
        rs_send[peer] = rows_of(part).astype(bf16)
        remote(rs_send.at[peer], rs_recv.at[me], r_send, r_recv, peer).start()

    def out_of(peer, count):
        span = pl.ds(pl.multiple_of(peer * dx, dx), count * dx)
        return jnp.dot(att, wo[:, span], preferred_element_type=f32)

    def project_out(i):
        first = base_of(i)
        part = out_of(first, per)
        for u in range(per):
            send_part(first + u, part[:, u * dx : (u + 1) * dx])

    def project_far(j, carry):
        if groups == 4:
            middle = (me // per + me // (2 * per)) % 2
            project_out(3 - j - middle * (1 - 2 * j))
        else:
            project_out(groups - 1 - j)
        return carry

    lax.fori_loop(0, groups - 2, project_far, 0)
    near = [(base_of(1), per), (half_of(1) // dx, half)]
    parts = [(first, count, out_of(first, count)) for first, count in near]
    for first, count, part in parts:
        for u in range(count):
            send_part(first + u, part[:, u * dx : (u + 1) * dx])
    mate = partner(me, 1, n)
    part, own = out_of(mate, 1), rows_of(out_of(me, 1))
    send_part(mate, part)

    all_received(rs_recv, r_send, r_recv)
    total = own
    if unrolled:
        for k in range(1, n):
            total = total + rs_recv[partner(me, k, n)].astype(f32)
    else:
        total = lax.fori_loop(
            1, n, lambda k, t: t + rs_recv[partner(me, k, n)].astype(f32), total
        )
    out_ref[...] = total.astype(bf16)

    all_sent(stats, t_send, t_recv)
    all_sent(xg, x_send, x_recv.at[0])
    all_sent(qg, q_send, q_recv)
    all_sent(so, o_send, o_recv)
    all_sent(sl, l_send, l_recv)
    all_sent(rs_send, r_send, r_recv)


def hand_over(result_ref, scale_ref, out_ref, token_scale_ref):
    out_ref[...] = result_ref[...]
    token_scale_ref[...] = scale_ref[...]


def on_device(n, hidden_in, norm_gain, w_qkv, w_out, key_cache, value_cache, lengths, positions):
    batch, dx = hidden_in.shape
    cw = w_qkv.shape[1]
    own_rows = w_out.shape[0] // HEAD_SIZE * batch
    total_heads = QUERY_HEADS + 2 * KEY_VALUE_HEADS
    widest = max(d * cw % LANES for d in range(n)) + cw
    blocks = rounded_up(widest, LANES) // LANES
    pieces = dx // LANES
    x_height = rounded_up(pieces * batch, 8) + rounded_up(pieces, 8)
    half = HEAD_SIZE // 2
    freq = np.float32(500000.0) ** (
        -(np.arange(half, dtype=np.float32) * np.float32(2.0)) / np.float32(HEAD_SIZE)
    )
    freq = jnp.asarray(np.tile(freq.astype(np.float32), 2)[None, :])
    bf16, f32 = jnp.bfloat16, jnp.float32
    dma = pltpu.SemaphoreType.DMA
    hbm = pl.BlockSpec(memory_space=pl.ANY)
    vmem = pl.BlockSpec(memory_space=pltpu.VMEM)
    out, token_scale = pl.pallas_call(
        functools.partial(kernel, n),
        out_shape=(
            pltpu.VMEM((pieces * batch, LANES), bf16),
            pltpu.VMEM((1, batch), f32),
        ),
        in_specs=[hbm] * 9,
        out_specs=(vmem, vmem),
        scratch_shapes=[
            pltpu.VMEM((n, x_height, LANES), bf16),
            pltpu.VMEM((n // 2, batch, 2 * dx), bf16),
            pltpu.VMEM((cw, n * dx), bf16),
            pltpu.VMEM(((n - 4) * dx, cw // LANES * LANES), bf16),
            pltpu.VMEM((4 * dx, cw // LANES * LANES), bf16),
            pltpu.VMEM((w_out.shape[0], n * dx), bf16),
            pltpu.VMEM(key_cache.shape, bf16),
            pltpu.VMEM((batch, key_cache.shape[2], key_cache.shape[1]), bf16),
            pltpu.VMEM(value_cache.shape, bf16),
            pltpu.VMEM((n, 1, LANES), f32),
            pltpu.VMEM((n, batch, blocks * LANES), bf16),
            pltpu.VMEM((total_heads * batch, HEAD_SIZE), f32),
            pltpu.VMEM((2, QUERY_HEADS * batch, HEAD_SIZE), f32),
            pltpu.VMEM((n, own_rows, LANES), bf16),
            pltpu.VMEM((n, own_rows, LANES), bf16),
            pltpu.VMEM((n, 1, LANES), f32),
            pltpu.VMEM((n, 1, LANES), f32),
            pltpu.VMEM((n, pieces * batch, LANES), bf16),
            pltpu.VMEM((n, pieces * batch, LANES), bf16),
            pltpu.SMEM((batch,), jnp.int32),
            pltpu.SMEM((batch,), jnp.int32),
            pltpu.VMEM((1, LANES), f32),
            dma((5,)),
            dma((n // 2,)),
            dma((n // 4,)),
            dma((2,)),
            dma(()),
            dma(()),
            dma(()),
            dma((n // 4,)),
        ]
        + [dma(())] * 8,
        compiler_params=pltpu.CompilerParams(
            collective_id=0, has_side_effects=True, vmem_limit_bytes=60 * 1024 * 1024
        ),
        name="decode",
    )(
        hidden_in.reshape(batch, pieces, LANES).transpose(1, 0, 2).reshape(-1, LANES),
        norm_gain.reshape(dx // LANES, LANES),
        w_qkv.T,
        w_out,
        key_cache,
        value_cache,
        lengths,
        positions,
        freq,
    )
    out = pltpu.with_memory_space_constraint(out, pltpu.VMEM)
    token_scale = pltpu.with_memory_space_constraint(token_scale, pltpu.VMEM)
    out, token_scale = pl.pallas_call(
        hand_over,
        out_shape=(
            jax.ShapeDtypeStruct(out.shape, out.dtype),
            jax.ShapeDtypeStruct(token_scale.shape, token_scale.dtype),
        ),
        in_specs=[vmem, vmem],
        out_specs=(vmem, vmem),
        name="hand_over",
    )(out, token_scale)
    out = out.reshape(pieces, batch, LANES).transpose(1, 0, 2).reshape(batch, dx)
    return out, token_scale.reshape(batch)


def solution(mesh):
    placed = (
        P("replica", "tp"),
        P("tp"),
        P(None, "tp"),
        P("tp", None),
        P("replica", "tp", None),
        P("replica", "tp", None),
        P("replica"),
        P("replica"),
    )
    return jax.shard_map(
        functools.partial(on_device, mesh.shape["tp"]),
        mesh=mesh,
        in_specs=placed,
        out_specs=(P("replica", "tp"), P("replica")),
        check_vma=False,
    )
```

```python
import functools

import jax
import jax.numpy as jnp
import numpy as np
from jax import lax
from jax.experimental import pallas as pl
from jax.experimental.pallas import tpu as pltpu
from jax.sharding import PartitionSpec as P

QUERY_HEADS = 64
KEY_VALUE_HEADS = 4
HEAD_SIZE = 128
LANES = 128


def rounded_up(value, step):
    return (value + step - 1) // step * step


def partner(me, k, n):
    peer = me
    bit = 1
    while bit < n:
        if isinstance(k, int):
            if k & bit:
                peer = peer + (bit - 2 * bit * ((me // bit) % 2))
        else:
            mine, flip = (me // bit) % 2, (k // bit) % 2
            peer = peer + bit * flip * (1 - 2 * mine)
        bit *= 2
    return peer


def kernel(
    n,
    hidden_hbm,
    gain_hbm,
    wq_hbm,
    wo_hbm,
    key_hbm,
    value_hbm,
    lens_hbm,
    pos_hbm,
    freq_hbm,
    out_ref,
    scale_ref,
    xg,
    quant,
    wq,
    wt,
    wz,
    wo,
    kv,
    kt,
    vv,
    stats,
    qg,
    heads,
    ordered,
    so,
    og,
    sl,
    lg,
    rs_send,
    rs_recv,
    lens_ref,
    pos_ref,
    freq_ref,
    local_sem,
    wq_sem,
    wo_sem,
    kv_sem,
    t_send,
    t_recv,
    x_send,
    x_recv,
    q_send,
    q_recv,
    o_send,
    o_recv,
    l_send,
    l_recv,
    r_send,
    r_recv,
):
    me = lax.axis_index("tp")
    dx = wo.shape[1] // n
    batch = lens_ref.shape[0]
    pieces = dx // LANES
    x_rows = pieces * batch
    gain_at = xg.shape[1] - rounded_up(pieces, 8)
    cw, width = wq_hbm.shape
    padded = qg.shape[2]
    own_rows = og.shape[1]
    own_heads = own_rows // batch
    positions = key_hbm.shape[1]
    group = QUERY_HEADS // KEY_VALUE_HEADS
    f32, bf16 = jnp.float32, jnp.bfloat16
    unrolled = n <= 16

    per = 4
    groups = n // per
    span_of = lambda base: pl.ds(pl.multiple_of(base * dx, per * dx), per * dx)

    def base_of(i):
        return partner(me, i * per, n) // per * per

    half = per // 2
    turned = wt.shape[1]

    def half_of(i):
        return pl.multiple_of(partner(me, i * half, n) // half * half * dx, half * dx)

    def wq_copy(i):
        span = pl.ds(half_of(i), half * dx)
        return pltpu.make_async_copy(wq_hbm.at[:, span], wq.at[:, span], wq_sem.at[i])

    def turn_into(ref, i, place):
        start = half_of(i)
        for j in range(half * dx // LANES):
            at = pl.multiple_of(start + j * LANES, LANES)
            to = pl.multiple_of(place * half * dx + j * LANES, LANES)
            ref[pl.ds(to, LANES), :] = wq[0:turned, pl.ds(at, LANES)].T

    def turn(i, count):
        for v in range(count):
            wq_copy(i + v).wait()
        for v in range(count):
            turn_into(wt, i + v, i + v)

    def turn_two(j, carry):
        turn(2 * j + 2, 2)
        return carry

    def wo_copy(i):
        span = span_of(base_of(i))
        return pltpu.make_async_copy(wo_hbm.at[:, span], wo.at[:, span], wo_sem)

    def remote(src, dst, send, recv, peer):
        return pltpu.make_async_remote_copy(
            src_ref=src,
            dst_ref=dst,
            send_sem=send,
            recv_sem=recv,
            device_id={"tp": peer},
            device_id_type=pl.DeviceIdType.MESH,
        )

    def far_group(j):
        if groups != 4:
            return groups - 1 - j
        middle = (me // per + me // (2 * per)) % 2
        return [3 - middle, 2 + middle, 1, 0][j]

    def far_first(act):
        if unrolled and groups == 4:
            for j in range(groups):
                for u in range(per - 1, -1, -1):
                    if j == groups - 1 and u == 0:
                        continue
                    k = far_group(j) * per + u
                    act(k, partner(me, k, n))
        elif unrolled:
            for k in range(n - 1, 0, -1):
                act(k, partner(me, k, n))
        else:

            def step(i, carry):
                act(n - 1 - i, partner(me, n - 1 - i, n))
                return carry

            lax.fori_loop(0, n - 1, step, 0)

    def near_first(act):
        if unrolled:
            for k in range(1, n):
                act(k, partner(me, k, n))
        else:

            def step(k, carry):
                act(k, partner(me, k, n))
                return carry

            lax.fori_loop(1, n, step, 0)

    def all_sent(ref, send, recv):
        part = ref.at[pl.ds(0, n - 1)]
        remote(part, part, send, recv, partner(me, 1, n)).wait_send()

    def all_received(ref, send, recv, count=n - 1):
        part = ref.at[pl.ds(0, count)]
        remote(part, part, send, recv, partner(me, 1, n)).wait_recv()

    small = [
        (hidden_hbm, xg.at[me, pl.ds(0, x_rows), :]),
        (gain_hbm, xg.at[me, pl.ds(gain_at, pieces), :]),
        (freq_hbm, freq_ref),
        (pos_hbm, pos_ref),
        (lens_hbm, lens_ref),
    ]
    small = [
        pltpu.make_async_copy(src, dst, local_sem.at[i]) for i, (src, dst) in enumerate(small)
    ]
    for copy in small:
        copy.start()

    barrier = pltpu.get_barrier_semaphore()
    def announce(peer):
        pl.semaphore_signal(
            barrier, inc=1, device_id={"tp": peer}, device_id_type=pl.DeviceIdType.MESH
        )

    if unrolled:
        for k in range(n - 1, 0, -1):
            announce(partner(me, k, n))
    else:
        far_first(lambda k, peer: announce(peer))
    copy_k = pltpu.make_async_copy(key_hbm, kv, kv_sem.at[0])
    copy_v = pltpu.make_async_copy(value_hbm, vv, kv_sem.at[1])

    for i in range(2 * groups):
        wq_copy(i).start()
    small[0].wait()
    small[1].wait()

    half8 = lax.broadcasted_iota(jnp.int32, (8, LANES), 0) // batch
    row4 = lax.broadcasted_iota(jnp.int32, (8, LANES), 0) % batch
    lane8 = lax.broadcasted_iota(jnp.int32, (8, LANES), 1)
    per8 = 8 // batch

    def gained(s):
        x = xg[s, 0:x_rows, :].astype(f32)
        g = xg[s, gain_at : gain_at + rounded_up(pieces, 8), :].astype(f32)
        xs, ys = [], []
        for j in range(x_rows // 8):
            x8 = x[8 * j : 8 * j + 8, :]
            g8 = jnp.zeros((8, LANES), f32)
            for u in range(per8):
                r = j * per8 + u
                g8 = jnp.where(half8 == u, g[r : r + 1, :], g8)
            xs.append(x8)
            ys.append(x8 * g8)
        return xs, ys

    xs, ys = gained(me)
    squares = sum(x8 * x8 for x8 in xs)
    peak = functools.reduce(jnp.maximum, [jnp.abs(y) for y in ys])
    squares = jnp.sum(squares, axis=-1, keepdims=True)
    peak = jnp.max(peak, axis=-1, keepdims=True)
    first = jnp.sum(jnp.where(lane8 == row4, squares, 0.0), axis=0, keepdims=True)
    second = jnp.max(jnp.where(lane8 == row4 + batch, peak, 0.0), axis=0, keepdims=True)
    stats[me] = jnp.where(lane8[0:1, :] < batch, first, second)


    pl.semaphore_wait(barrier, n - 1)

    far_first(
        lambda k, peer: remote(stats.at[me], stats.at[me], t_send, t_recv, peer).start()
    )
    def send_x(k, peer):
        remote(xg.at[me], xg.at[me], x_send, x_recv.at[k // per], peer).start()

    near_first(send_x)

    turn(0, 1)
    turn(1, 1)
    lax.fori_loop(0, groups - 2, turn_two, 0)
    all_received(stats, t_send, t_recv)
    if n % 8 == 0:
        rows = [stats[8 * i : 8 * i + 8, 0, :] for i in range(n // 8)]
        added = jnp.sum(sum(rows), axis=0, keepdims=True)
        largest = jnp.max(functools.reduce(jnp.maximum, rows), axis=0, keepdims=True)
    else:
        rows = [stats[i] for i in range(n)]
        added = sum(rows)
        largest = functools.reduce(jnp.maximum, rows)
    added = jnp.sum(jnp.where(lane8 == row4, added, 0.0), axis=-1, keepdims=True)
    largest = jnp.max(jnp.where(lane8 == row4 + batch, largest, 0.0), axis=-1, keepdims=True)
    rstd8 = lax.rsqrt(added / width + 1e-05)
    scale8 = (largest * rstd8 + 1e-06) / 448.0
    token_scale = scale8[0:batch, :]
    scale_ref[...] = jnp.sum(
        jnp.where((lane8 == row4) & (half8 == 0), scale8, 0.0), axis=0, keepdims=True
    )[:, 0:batch]
    rstd8 = jnp.broadcast_to(rstd8, (8, LANES))
    scale8 = jnp.broadcast_to(scale8, (8, LANES))

    copy_k.start()
    copy_v.start()
    for i in range(groups - 1, -1, -1):
        wo_copy(i).start()

    def project(i, carry, ref, place):
        acc, rest = carry
        for v in range(2):
            first = half_of(2 * i + v) // dx
            for u in range(half):
                _, ys = gained(first + u)
                rows = [y * rstd8 / scale8 for y in ys]
                flat = [row[w * batch : (w + 1) * batch, :] for row in rows for w in range(per8)]
                quant[2 * i + v, :, u * dx : (u + 1) * dx] = jnp.concatenate(
                    flat, axis=1
                ).astype(bf16)
        for v in range(2):
            x = quant[2 * i + v]
            to = pl.multiple_of((2 * place + v) * half * dx, half * dx)
            acc = acc + jnp.dot(x, ref[pl.ds(to, half * dx), :], preferred_element_type=f32)
            if turned < cw:
                rest = rest + lax.dot_general(
                    x,
                    wq[turned:cw, pl.ds(half_of(2 * i + v), half * dx)],
                    (((1,), (1,)), ((), ())),
                    preferred_element_type=f32,
                )
        return acc, rest

    def project_middle(i, carry):
        all_received(xg, x_send, x_recv.at[i], per)
        return project(i, carry, wt, i)

    carry = (jnp.zeros((batch, turned), f32), jnp.zeros((batch, cw - turned), f32))
    for i in range(2):
        wq_copy(2 * groups - 2 + i).wait()
        all_received(xg, x_send, x_recv.at[i], per if i else per - 1)
    for i in range(2):
        turn_into(wz, 2 * groups - 2 + i, i)
        carry = project(i, carry, wt, i)
    carry = lax.fori_loop(2, groups - 1, project_middle, carry)
    all_received(xg, x_send, x_recv.at[groups - 1], per)
    acc, rest = project(groups - 1, carry, wz, 0)
    if turned < cw:
        acc = jnp.concatenate([acc, rest], axis=1)
    proj = (acc * token_scale).astype(bf16).astype(f32)
    if padded > cw:
        proj = jnp.concatenate([proj, jnp.zeros((batch, padded - cw), f32)], axis=1)
    if cw % LANES:
        proj = pltpu.roll(proj, lax.rem(me * cw, LANES), 1)
    qg[me] = proj.astype(bf16)
    far_first(lambda k, peer: remote(qg.at[me], qg.at[me], q_send, q_recv, peer).start())
    for copy in small[2:]:
        copy.wait()
    place = jnp.zeros((8, LANES), f32)
    for b in range(batch):
        place = jnp.where(row4 == b, pos_ref[b].astype(f32), place)
    angle = place * freq_ref[...]
    cosine = jnp.cos(angle)
    sine = jnp.sin(angle)
    sine = jnp.where(lane8 < HEAD_SIZE // 2, -sine, sine)

    copy_k.wait()
    copy_v.wait()
    for b in range(batch):
        kt[b] = kv[b].T
    all_received(qg, q_send, q_recv)

    total_heads = QUERY_HEADS + 2 * KEY_VALUE_HEADS
    unpacked = [qg[d].astype(f32) for d in range(n)]
    for h in range(total_heads):
        piece = None
        for d in range(h * LANES // cw, (h * LANES + LANES - 1) // cw + 1):
            block = h - d * cw // LANES
            part = unpacked[d][:, block * LANES : (block + 1) * LANES]
            piece = part if piece is None else piece + part
        heads[h * batch : (h + 1) * batch, :] = piece

    inv = 1.0 / HEAD_SIZE**0.5

    def row_of(rows, b):
        return jnp.broadcast_to(rows[b : b + 1, :], (group, HEAD_SIZE))

    cosines = [row_of(cosine, b) for b in range(batch)]
    sines = [row_of(sine, b) for b in range(batch)]

    def rotated(rows, cosine, sine):
        return rows * cosine + pltpu.roll(rows, HEAD_SIZE // 2, 1) * sine

    spot = lax.broadcasted_iota(jnp.int32, (group, positions), 1) + me * positions
    masks = [jnp.where(spot < lens_ref[b], 0.0, -1e30) for b in range(batch)]
    units = [(g, b) for g in range(KEY_VALUE_HEADS) for b in range(batch)]

    def stacked(rows):
        return jnp.concatenate(rows, axis=0)

    valid = stacked([masks[b] for g, b in units]) == 0.0
    tokens = KEY_VALUE_HEADS * batch
    first = QUERY_HEADS * batch
    fresh_k = rotated(
        heads[first : first + tokens, :],
        jnp.tile(cosine, (tokens // 8, 1)),
        jnp.tile(sine, (tokens // 8, 1)),
    )
    fresh_v = heads[first + tokens : first + 2 * tokens, :]
    queries, scores = [], []
    for g, b in units:
        q = heads[pl.ds(g * group * batch + b, group, stride=batch), :]
        q = rotated(q, cosines[b], sines[b]).astype(bf16)
        keys = kt[b, g * HEAD_SIZE : (g + 1) * HEAD_SIZE, :]
        queries.append(q)
        scores.append(jnp.dot(q, keys, preferred_element_type=f32))
    s = stacked(scores) * inv
    top = jnp.max(jnp.where(valid, s, -1e30), axis=-1, keepdims=True)
    w = jnp.where(valid, jnp.exp(s - top), 0.0)
    total = jnp.sum(w, axis=-1, keepdims=True)
    w = w.astype(bf16)
    o = stacked(
        [
            jnp.dot(
                w[i * group : (i + 1) * group, :],
                vv[b, :, g * HEAD_SIZE : (g + 1) * HEAD_SIZE],
                preferred_element_type=f32,
            )
            for i, (g, b) in enumerate(units)
        ]
    )
    k_new = stacked([row_of(fresh_k, g * batch + b) for g, b in units])
    v_new = stacked([row_of(fresh_v, g * batch + b) for g, b in units])
    s_new = jnp.sum(stacked(queries).astype(f32) * k_new, axis=-1, keepdims=True) * inv
    s_new = jnp.where(me == 0, s_new, -1e30)
    top_new = jnp.maximum(top, s_new)
    keep = jnp.exp(top - top_new)
    fresh = jnp.where(me == 0, jnp.exp(s_new - top_new), 0.0)
    total = total * keep + fresh
    o = o * keep + fresh * v_new
    some = total > 0.0
    safe = jnp.where(some, total, 1.0)
    o = o / safe
    lse = jnp.where(some, top_new + jnp.log(safe), -1e30)
    lse = jnp.broadcast_to(lse, o.shape)
    for i, (g, b) in enumerate(units):
        spread = pl.ds(g * group * batch + b, group, stride=batch)
        ordered[0, spread, :] = o[i * group : (i + 1) * group, :]
        ordered[1, spread, :] = lse[i * group : (i + 1) * group, :]
    own_lane = lax.broadcasted_iota(jnp.int32, (own_rows, LANES), 1)
    own_row = lax.broadcasted_iota(jnp.int32, (own_rows, LANES), 0)
    diagonal = own_lane == own_row
    for e in range(n):
        rows = slice(e * own_rows, (e + 1) * own_rows)
        so[e] = ordered[0, rows, :].astype(bf16)
        sl[e] = jnp.sum(jnp.where(diagonal, ordered[1, rows, :], 0.0), axis=0, keepdims=True)

    def send_o(k, peer):
        remote(so.at[peer], og.at[me], o_send, o_recv, peer).start()
        remote(sl.at[peer], lg.at[me], l_send, l_recv, peer).start()

    far_first(send_o)
    og[me] = so[me]
    lg[me] = sl[me]
    pltpu.make_async_copy(wo_hbm, wo, wo_sem).wait()

    all_received(lg, l_send, l_recv)
    all_received(og, o_send, o_recv)

    lses = [
        jnp.sum(jnp.where(diagonal, lg[s], 0.0), axis=-1, keepdims=True) for s in range(n)
    ]
    best = functools.reduce(jnp.maximum, lses)
    den = jnp.zeros_like(best)
    num = jnp.zeros((own_rows, LANES), f32)
    for s in range(n):
        share = jnp.exp(lses[s] - best)
        den = den + share
        num = num + share * og[s].astype(f32)
    att = num / den
    att = jnp.concatenate(
        [att[j * batch : (j + 1) * batch, :] for j in range(own_heads)], axis=1
    ).astype(bf16)

    def rows_of(part):
        return jnp.concatenate(
            [part[:, j * LANES : (j + 1) * LANES] for j in range(pieces)], axis=0
        )

    def send_part(peer, part):
        rs_send[peer] = rows_of(part).astype(bf16)
        remote(rs_send.at[peer], rs_recv.at[me], r_send, r_recv, peer).start()

    def out_of(peer, count):
        span = pl.ds(pl.multiple_of(peer * dx, dx), count * dx)
        return jnp.dot(att, wo[:, span], preferred_element_type=f32)

    def project_out(i):
        first = base_of(i)
        part = out_of(first, per)
        for u in range(per):
            send_part(first + u, part[:, u * dx : (u + 1) * dx])

    def project_far(j, carry):
        if groups == 4:
            middle = (me // per + me // (2 * per)) % 2
            project_out(3 - j - middle * (1 - 2 * j))
        else:
            project_out(groups - 1 - j)
        return carry

    lax.fori_loop(0, groups - 2, project_far, 0)
    near = [(base_of(1), per), (half_of(1) // dx, half)]
    parts = [(first, count, out_of(first, count)) for first, count in near]
    for first, count, part in parts:
        for u in range(count):
            send_part(first + u, part[:, u * dx : (u + 1) * dx])
    mate = partner(me, 1, n)
    part, own = out_of(mate, 1), rows_of(out_of(me, 1))
    send_part(mate, part)

    all_received(rs_recv, r_send, r_recv)
    total = own
    if unrolled:
        for k in range(1, n):
            total = total + rs_recv[partner(me, k, n)].astype(f32)
    else:
        total = lax.fori_loop(
            1, n, lambda k, t: t + rs_recv[partner(me, k, n)].astype(f32), total
        )
    out_ref[...] = total.astype(bf16)

    all_sent(stats, t_send, t_recv)
    all_sent(xg, x_send, x_recv.at[0])
    all_sent(qg, q_send, q_recv)
    all_sent(so, o_send, o_recv)
    all_sent(sl, l_send, l_recv)
    all_sent(rs_send, r_send, r_recv)


def hand_over(result_ref, scale_ref, out_ref, token_scale_ref):
    out_ref[...] = result_ref[...]
    token_scale_ref[...] = scale_ref[...]


def on_device(n, hidden_in, norm_gain, w_qkv, w_out, key_cache, value_cache, lengths, positions):
    batch, dx = hidden_in.shape
    cw = w_qkv.shape[1]
    own_rows = w_out.shape[0] // HEAD_SIZE * batch
    total_heads = QUERY_HEADS + 2 * KEY_VALUE_HEADS
    widest = max(d * cw % LANES for d in range(n)) + cw
    blocks = rounded_up(widest, LANES) // LANES
    pieces = dx // LANES
    x_height = rounded_up(pieces * batch, 8) + rounded_up(pieces, 8)
    half = HEAD_SIZE // 2
    freq = np.float32(500000.0) ** (
        -(np.arange(half, dtype=np.float32) * np.float32(2.0)) / np.float32(HEAD_SIZE)
    )
    freq = jnp.asarray(np.tile(freq.astype(np.float32), 2)[None, :])
    bf16, f32 = jnp.bfloat16, jnp.float32
    dma = pltpu.SemaphoreType.DMA
    hbm = pl.BlockSpec(memory_space=pl.ANY)
    vmem = pl.BlockSpec(memory_space=pltpu.VMEM)
    out, token_scale = pl.pallas_call(
        functools.partial(kernel, n),
        out_shape=(
            pltpu.VMEM((pieces * batch, LANES), bf16),
            pltpu.VMEM((1, batch), f32),
        ),
        in_specs=[hbm] * 9,
        out_specs=(vmem, vmem),
        scratch_shapes=[
            pltpu.VMEM((n, x_height, LANES), bf16),
            pltpu.VMEM((n // 2, batch, 2 * dx), bf16),
            pltpu.VMEM((cw, n * dx), bf16),
            pltpu.VMEM(((n - 4) * dx, cw // LANES * LANES), bf16),
            pltpu.VMEM((4 * dx, cw // LANES * LANES), bf16),
            pltpu.VMEM((w_out.shape[0], n * dx), bf16),
            pltpu.VMEM(key_cache.shape, bf16),
            pltpu.VMEM((batch, key_cache.shape[2], key_cache.shape[1]), bf16),
            pltpu.VMEM(value_cache.shape, bf16),
            pltpu.VMEM((n, 1, LANES), f32),
            pltpu.VMEM((n, batch, blocks * LANES), bf16),
            pltpu.VMEM((total_heads * batch, HEAD_SIZE), f32),
            pltpu.VMEM((2, QUERY_HEADS * batch, HEAD_SIZE), f32),
            pltpu.VMEM((n, own_rows, LANES), bf16),
            pltpu.VMEM((n, own_rows, LANES), bf16),
            pltpu.VMEM((n, 1, LANES), f32),
            pltpu.VMEM((n, 1, LANES), f32),
            pltpu.VMEM((n, pieces * batch, LANES), bf16),
            pltpu.VMEM((n, pieces * batch, LANES), bf16),
            pltpu.SMEM((batch,), jnp.int32),
            pltpu.SMEM((batch,), jnp.int32),
            pltpu.VMEM((1, LANES), f32),
            dma((5,)),
            dma((n // 2,)),
            dma(()),
            dma((2,)),
            dma(()),
            dma(()),
            dma(()),
            dma((n // 4,)),
        ]
        + [dma(())] * 8,
        compiler_params=pltpu.CompilerParams(
            collective_id=0, has_side_effects=True, vmem_limit_bytes=60 * 1024 * 1024
        ),
        name="decode",
    )(
        hidden_in.reshape(batch, pieces, LANES).transpose(1, 0, 2).reshape(-1, LANES),
        norm_gain.reshape(dx // LANES, LANES),
        w_qkv.T,
        w_out,
        key_cache,
        value_cache,
        lengths,
        positions,
        freq,
    )
    out = pltpu.with_memory_space_constraint(out, pltpu.VMEM)
    token_scale = pltpu.with_memory_space_constraint(token_scale, pltpu.VMEM)
    out, token_scale = pl.pallas_call(
        hand_over,
        out_shape=(
            jax.ShapeDtypeStruct(out.shape, out.dtype),
            jax.ShapeDtypeStruct(token_scale.shape, token_scale.dtype),
        ),
        in_specs=[vmem, vmem],
        out_specs=(vmem, vmem),
        name="hand_over",
    )(out, token_scale)
    out = out.reshape(pieces, batch, LANES).transpose(1, 0, 2).reshape(batch, dx)
    return out, token_scale.reshape(batch)


def solution(mesh):
    placed = (
        P("replica", "tp"),
        P("tp"),
        P(None, "tp"),
        P("tp", None),
        P("replica", "tp", None),
        P("replica", "tp", None),
        P("replica"),
        P("replica"),
    )
    return jax.shard_map(
        functools.partial(on_device, mesh.shape["tp"]),
        mesh=mesh,
        in_specs=placed,
        out_specs=(P("replica", "tp"), P("replica")),
        check_vma=False,
    )
```
